32 devices in a mesh: ctx: 8 (over y, x, core), head: 4 (over z).
Axes of the slice: x: 2, y: 2, z: 4, core: 2. Of those that a mesh axis runs over, the one named last changes fastest.
Arguments:
- tokens: bfloat16 [2, 2048, 2048], P(None, 'ctx'), may hold values from -6 to 6
- w_qkv: bfloat16 [2048, 4, 1536], P(None, 'head'), as said below
- w_rate: bfloat16 [2048, 4], P(None, 'head'), may hold values from -0.125 to 0.125
- w_out: bfloat16 [4, 512, 2048], P('head'), may hold values from -0.125 to 0.125
- fw_gain: float32 [4, 512], P('head'), may hold values from 0.25 to 1.75
- fast_first: float32 [4, 512, 512], P('head'), may hold values from -0.25 to 0.25
- fast_third: float32 [4, 512, 512], P('head'), may hold values from -0.25 to 0.25
- fast_second: float32 [4, 512, 512], P('head'), may hold values from -0.25 to 0.25
Outputs:
- mixed: bfloat16 [2, 2048, 2048], P(None, 'ctx', 'head')
- new_first: float32 [4, 512, 512], P('head')
- new_third: float32 [4, 512, 512], P('head')
- new_second: float32 [4, 512, 512], P('head')
The draws below stay inside these ranges and needn't reach their ends.
Inputs may be any that keep to these rules, and one draw needn't show every extreme that they name: `w_qkv`: A projection scaled by its fan-in 2048.
All inputs are finite; a program needn't handle non-finite values.
Results may differ from the reference program's by a relative error of at most 0.039.
Values may be sent and summed in bfloat16 or wider, within the bound.
A program may use at most 128 MiB of HBM per device.

```python
import jax
import jax.numpy as jnp
from jax import lax

D = 2048
HEADS = 4
DH = 512
FH = 512
TOK_DEV = 256
WINDOW = 2048
BLOCKS = 2
NS_STEPS = 5
BLOCK = 2048


def draw_tokens(key, part):
    base = jax.random.normal(jax.random.fold_in(key, 11), (BLOCKS, BLOCK, D), jnp.float32)
    base = jnp.clip(base, -6.0, 6.0)
    return base.astype(jnp.bfloat16)


def draw_w_qkv(key, part):
    base = jax.random.normal(jax.random.fold_in(key, 23), (D, HEADS, 3 * DH), jnp.float32)
    base = jnp.clip(base, -6.0, 6.0) * D ** (-0.5)
    return base.astype(jnp.bfloat16)


def level_of(key, shape, pieces, low, high):
    loudness, own = 1.0, jax.random.fold_in(key, 6)
    for axis_at, parts in pieces:
        steps = jnp.exp(jax.random.uniform(jax.random.fold_in(own, axis_at), (parts,), jnp.float32, low / len(pieces), high / len(pieces)))
        loudness = loudness * jnp.repeat(steps, shape[axis_at] // parts).reshape([-1 if axis == axis_at else 1 for axis in range(len(shape))])
    return loudness


def scatter_about(rng, shape, spread, bound, cuts=(), held_as=jnp.bfloat16):
    drawn = spread * jax.random.normal(rng, shape, jnp.float32)
    if cuts:
        drawn = drawn * level_of(rng, shape, cuts, -0.22, 0.18)
    return jnp.clip(drawn, -bound, bound).astype(held_as)


def setup_inputs(seed: int = 0) -> dict:
    key_list = jax.random.split(jax.random.key(seed), 9)
    tokens = draw_tokens(jax.random.fold_in(key_list[8], 71), 0)
    w_qkv = draw_w_qkv(jax.random.fold_in(key_list[8], 71), 0)
    w_rate = scatter_about(key_list[2], (D, HEADS), D ** -0.5, 0.125, ((1, 4),))
    w_out = scatter_about(key_list[3], (HEADS, DH, D), D ** -0.5, 0.125, ((0, 4),))
    fw_gain = jnp.clip(1.0 + 0.15 * jax.random.normal(key_list[4], (HEADS, DH), jnp.float32), 0.25, 1.75)
    fast_first = scatter_about(key_list[5], (HEADS, DH, FH), DH ** -0.5, 0.25, ((0, 4),), jnp.float32)
    fast_third = scatter_about(key_list[6], (HEADS, DH, FH), DH ** -0.5, 0.25, ((0, 4),), jnp.float32)
    fast_second = scatter_about(key_list[7], (HEADS, FH, DH), FH ** -0.5, 0.25, ((0, 4),), jnp.float32)
    return dict(tokens=tokens, w_qkv=w_qkv, w_rate=w_rate, w_out=w_out, fw_gain=fw_gain, fast_first=fast_first, fast_third=fast_third, fast_second=fast_second)


coeff_a = 3.4445
coeff_b = -4.775
coeff_c = 2.0315
fast_step = 0.5
norm_eps = 1e-06

def inner_rows(left, right):
    return lax.dot_general(left, right, (((0,), (0,)), ((), ())), preferred_element_type=jnp.float32)

def silu_grad(hidden):
    sigma = jax.nn.sigmoid(hidden)
    return sigma * (1.0 + hidden * (1.0 - sigma))

def narrow(weights):
    return tuple((weight.astype(jnp.bfloat16) for weight in weights))

def fast_apply(queries, narrowed):
    hidden_one = jnp.dot(queries, narrowed[0], preferred_element_type=jnp.float32)
    hidden_three = jnp.dot(queries, narrowed[1], preferred_element_type=jnp.float32)
    activ = (jax.nn.silu(hidden_one) * hidden_three).astype(jnp.bfloat16)
    return jnp.dot(activ, narrowed[2], preferred_element_type=jnp.float32)

def fast_grads(keys, values, rates, narrowed):
    hidden_one = jnp.dot(keys, narrowed[0], preferred_element_type=jnp.float32)
    hidden_three = jnp.dot(keys, narrowed[1], preferred_element_type=jnp.float32)
    activ = (jax.nn.silu(hidden_one) * hidden_three).astype(jnp.bfloat16)
    target = (-rates[:, None] * values.astype(jnp.float32)).astype(jnp.bfloat16)
    grad_second = inner_rows(activ, target)
    dactiv = lax.dot_general(target, narrowed[2], (((1,), (1,)), ((), ())), preferred_element_type=jnp.float32)
    d_first = (dactiv * hidden_three * silu_grad(hidden_one)).astype(jnp.bfloat16)
    d_third = (dactiv * jax.nn.silu(hidden_one)).astype(jnp.bfloat16)
    return (inner_rows(keys, d_first), inner_rows(keys, d_third), grad_second)

def gram_of(current):
    return lax.dot_general(current, current, (((0,), (0,)), ((), ())), precision=lax.Precision.HIGHEST, preferred_element_type=jnp.float32)

def ns_update(current, gram):
    poly = coeff_b * gram + coeff_c * jnp.dot(gram, gram, precision=lax.Precision.HIGHEST)
    return coeff_a * current + jnp.dot(current, poly, precision=lax.Precision.HIGHEST)

def orthogonalize(grad):
    current = grad / jnp.sqrt(jnp.sum(grad * grad) + norm_eps)
    for step_num in range(NS_STEPS):
        current = ns_update(current, gram_of(current))
    return current

def window_softmax(query_rows, key_rows, value_rows, first_key):
    row_count = query_rows.shape[0]
    key_span = key_rows.shape[0]
    window_len = key_span - row_count
    scores = lax.dot_general(query_rows, key_rows, (((1,), (1,)), ((), ())), preferred_element_type=jnp.float32)
    scores = scores * query_rows.shape[1] ** (-0.5)
    offsets = window_len + lax.broadcasted_iota(jnp.int32, (row_count, key_span), 0) - lax.broadcasted_iota(jnp.int32, (row_count, key_span), 1)
    positions = first_key + lax.broadcasted_iota(jnp.int32, (row_count, key_span), 1)
    allowed = (offsets >= 0) & (offsets < window_len) & (positions >= 0)
    scores = jnp.where(allowed, scores, -1e+30)
    highest = lax.optimization_barrier(jnp.max(scores, axis=1, keepdims=True))
    weights = jnp.exp(scores - highest)
    weights = (weights / lax.optimization_barrier(jnp.sum(weights, axis=1, keepdims=True))).astype(jnp.bfloat16)
    return jnp.dot(weights, value_rows, preferred_element_type=jnp.float32)

def attend(queries, keys, values):
    total_rows = queries.shape[0]
    pad_keys = jnp.pad(keys, ((WINDOW, 0), (0, 0)))
    pad_values = jnp.pad(values, ((WINDOW, 0), (0, 0)))

    def one_block(block_num):
        start = (block_num * TOK_DEV).astype(jnp.int32)
        query_rows = lax.dynamic_slice_in_dim(queries, start, TOK_DEV, 0)
        key_rows = lax.dynamic_slice_in_dim(pad_keys, start, WINDOW + TOK_DEV, 0)
        value_rows = lax.dynamic_slice_in_dim(pad_values, start, WINDOW + TOK_DEV, 0)
        return window_softmax(query_rows, key_rows, value_rows, start - WINDOW)
    outputs = lax.map(one_block, jnp.arange(total_rows // TOK_DEV, dtype=jnp.int32))
    return outputs.reshape(total_rows, DH)

def reference(tokens, w_qkv, w_rate, w_out, fw_gain, fast_first, fast_third, fast_second):
    flat = tokens.reshape(BLOCKS * BLOCK, D)
    projected = jnp.dot(flat, w_qkv.reshape(D, HEADS * 3 * DH), preferred_element_type=jnp.float32).astype(jnp.bfloat16)
    projected = projected.reshape(BLOCKS * BLOCK, HEADS, 3, DH)
    rates = jax.nn.softplus(jnp.dot(flat, w_rate, preferred_element_type=jnp.float32))
    mixed = jnp.zeros((BLOCKS * BLOCK, D), jnp.float32)
    final_first = []
    final_third = []
    final_second = []
    for head_num in range(HEADS):
        queries = projected[:, head_num, 0]
        keys = projected[:, head_num, 1]
        values = projected[:, head_num, 2]
        attended = attend(queries, keys, values)
        current = (fast_first[head_num], fast_third[head_num], fast_second[head_num])
        outputs = []
        for block_num in range(BLOCKS):
            lower = block_num * BLOCK
            upper = lower + BLOCK
            outputs.append(fast_apply(queries[lower:upper], narrow(current)))
            if block_num + 1 < BLOCKS:
                grads = fast_grads(keys[lower:upper], values[lower:upper], rates[lower:upper, head_num], narrow(current))
                current = tuple((weight - fast_step * orthogonalize(grad) for weight, grad in zip(current, grads)))
        fast_out = jnp.concatenate(outputs, axis=0)
        normed = fast_out * lax.rsqrt(lax.optimization_barrier(jnp.mean(fast_out * fast_out, axis=1, keepdims=True)) + norm_eps) * fw_gain[head_num]
        combined = (attended + normed).astype(jnp.bfloat16)
        mixed = mixed + jnp.dot(combined, w_out[head_num], preferred_element_type=jnp.float32)
        final_first.append(current[0])
        final_third.append(current[1])
        final_second.append(current[2])
    mixed = mixed.astype(jnp.bfloat16).reshape(BLOCKS, BLOCK, D)
    return (mixed, jnp.stack(final_first), jnp.stack(final_third), jnp.stack(final_second))
```

```python
import functools

import jax
import jax.numpy as jnp
from jax import lax
from jax.experimental import pallas as pl
from jax.experimental.pallas import tpu as pltpu
from jax.sharding import PartitionSpec as P

WINDOW = 2048
NS_STEPS = 5

coeff_a = 3.4445
coeff_b = -4.775
coeff_c = 2.0315
fast_step = 0.5
norm_eps = 1e-06
LOG2E = 1.4426950408889634
NEG = -1e30
BF = jnp.bfloat16
F32 = jnp.float32
VMEM = pl.BlockSpec(memory_space=pltpu.VMEM)
ANY = pl.BlockSpec(memory_space=pl.ANY)
LANES = 128


def mm(left, right, dims):
    return lax.dot_general(left, right, (dims, ((), ())), preferred_element_type=F32)


def nn(left, right):
    return mm(left, right, ((1,), (0,)))


def nt(left, right):
    return mm(left, right, ((1,), (1,)))


def tn(left, right):
    return mm(left, right, ((0,), (0,)))


def cross_bits(n, sub):
    bits = [1 << i for i in range(1, n.bit_length() - 1)]
    return bits if sub == 0 else bits[::-1]


def remote(src, dst, send, recv, axis, peer):
    return pltpu.make_async_remote_copy(
        src_ref=src,
        dst_ref=dst,
        send_sem=send,
        recv_sem=recv,
        device_id={axis: peer},
        device_id_type=pl.DeviceIdType.MESH,
    )


def layer_kernel(
    n, nh, rows,
    tok_h, w_h, wr, f1_h, f3_h, f2_h, gain, wo_h,
    mixed_h, o1_h, o3_h, o2_h,
    tok, w, f_v, fb, wo, wp, q_v, every, rates,
    grad, g_out, g_in,
    m_s, l_s, acc, normed, comb, part_in, res,
    load, k_send, k_recv, s_send, s_recv, g_send, g_recv, x_send, x_recv,
    w_send, w_recv, c_send, c_recv, p_send, p_recv, out_sem,
):
    me = lax.axis_index("ctx")
    hme = lax.axis_index("head")
    dh = q_v.shape[1]
    cols = wo.shape[2]
    reach = WINDOW // rows
    scale = dh ** (-0.5) * LOG2E
    half = rows // 2
    core = lax.rem(me, 2)
    fine = n <= 8
    evens = sorted(range(2, n, 2), key=lambda c: (bin(c).count("1"), c))
    hpair = hme // 2
    hodd = lax.rem(hme, 2)
    mate = hme + 1 - 2 * hodd

    def fetch(i, src, dst):
        copy = pltpu.make_async_copy(src, dst, load.at[i])
        copy.start()
        return copy

    first, second = pl.ds(0, rows), pl.ds(rows, rows)
    in_tok0 = fetch(0, tok_h.at[first], tok.at[first])
    in_k = fetch(1, w_h.at[:, pl.ds(dh, dh)], w.at[1])
    in_v = fetch(2, w_h.at[:, pl.ds(2 * dh, dh)], w.at[2])
    in_tok1 = fetch(3, tok_h.at[second], tok.at[second])
    in_q = fetch(4, w_h.at[:, pl.ds(0, dh)], w.at[0])
    in_f = [fetch(5 + i, f, f_v.at[i]) for i, f in enumerate((f1_h, f3_h, f2_h))]
    in_wo = [
        fetch(8 + t, wo_h.at[:, pl.ds(t * cols, cols)], wo.at[t]) for t in range(nh)
    ]

    barrier = pltpu.get_barrier_semaphore()
    peers = [1] + evens
    for c in peers:
        pl.semaphore_signal(
            barrier, inc=1, device_id={"ctx": me ^ c}, device_id_type=pl.DeviceIdType.MESH
        )
    for r in range(1, nh):
        pl.semaphore_signal(
            barrier,
            inc=1,
            device_id={"head": lax.rem(hme + r, nh)},
            device_id_type=pl.DeviceIdType.MESH,
        )

    started = []

    def go(copy):
        copy.start()
        started.append(copy)

    def place(p):
        return pl.ds((p // 2) * rows + (p % 2) * half, half)

    def kv_copy(p, c, bit):
        ref = every.at[me ^ c, place(p)]
        return remote(ref, ref, k_send.at[p, c | bit], k_recv.at[p, c | bit], "ctx", me ^ bit)

    def kv_wait(p, c):
        ref = every.at[me ^ c, place(p)]
        remote(ref, ref, k_send.at[p, c], k_recv.at[p, c], "ctx", me ^ (c & -c)).wait_recv()

    def pass_on(p, c):
        order = cross_bits(n, p % 2)
        last = max(i for i, bit in enumerate(order) if c & bit)
        for bit in order[last + 1 :]:
            go(kv_copy(p, c, bit))
        go(kv_copy(p, c, 1))

    def send_own(b):
        lists = [cross_bits(n, sub) for sub in range(2)]
        for pair in zip(*lists):
            for sub in range(2):
                go(kv_copy(2 * b + sub, 0, pair[sub]))
        for sub in range(2):
            go(kv_copy(2 * b + sub, 0, 1))

    def first_hops(b):
        for sub in range(2):
            c = cross_bits(n, sub)[0]
            kv_wait(2 * b + sub, c)
            pass_on(2 * b + sub, c)

    def near_hops(b):
        for sub in range(2):
            for c in evens:
                if c & (c - 1) == 0 and c != cross_bits(n, sub)[0]:
                    kv_wait(2 * b + sub, c)
                    pass_on(2 * b + sub, c)

    def far_hops(b):
        for c in evens:
            if c & (c - 1):
                for sub in range(2):
                    kv_wait(2 * b + sub, c)
                    pass_on(2 * b + sub, c)

    def from_mate(b, c):
        for sub in range(2):
            kv_wait(2 * b + sub, c)

    in_tok0.wait()
    in_k.wait()
    every[me, :rows, :dh] = nn(tok[:rows], w[1]).astype(BF)
    in_v.wait()
    every[me, :rows, dh:] = nn(tok[:rows], w[2]).astype(BF)
    pl.semaphore_wait(barrier, len(peers) + nh - 1)
    send_own(0)

    logit = nt(jnp.broadcast_to(wr[...], (8, wr.shape[1])), tok[:rows])
    rates[0] = jnp.maximum(logit, 0.0) + jnp.log1p(jnp.exp(-jnp.abs(logit)))
    for c in evens:
        go(
            remote(
                rates.at[0], rates.at[c // 2], s_send.at[c // 2], s_recv.at[c // 2], "ctx", me ^ c
            )
        )

    def rate_wait(c):
        ref = rates.at[c // 2]
        remote(ref, ref, s_send.at[c // 2], s_recv.at[c // 2], "ctx", me ^ c).wait_recv()

    def crosses(h, t):
        odd = lax.rem(h, 2)
        up = (odd == 1) & (t // 2 > h // 2)
        down = (odd == 0) & (t // 2 < h // 2)
        return up | down

    def wo_copy(t):
        return remote(
            wo_h.at[:, pl.ds(t * cols, cols)], wp.at[t], w_send.at[t], w_recv.at[t], "head", mate
        )

    for t in range(nh):

        @pl.when((mate == t) | crosses(mate, t))
        def _():
            wo_copy(t).start()

    in_tok1.wait()
    every[me, rows:, :dh] = nn(tok[rows:], w[1]).astype(BF)
    every[me, rows:, dh:] = nn(tok[rows:], w[2]).astype(BF)
    in_q.wait()
    q_v[...] = nn(tok[...], w[0]).astype(BF)
    for i in range(3):
        in_f[i].wait()
        fb[i] = f_v[i].astype(BF)

    def gradients(s, at, slot, add):
        keys = every[s, :rows, :dh]
        vals = every[s, :rows, dh:]
        rate = jnp.transpose(rates[at])[:, :1]
        target = (-rate * vals.astype(F32)).astype(BF)
        h1 = nn(keys, fb[0])
        h3 = nn(keys, fb[1])
        sig = jax.nn.sigmoid(h1)
        silu = h1 * sig
        act = (silu * h3).astype(BF)
        dact = nt(target, fb[2])
        d1 = (dact * h3 * (sig * (1.0 + h1 * (1.0 - sig)))).astype(BF)
        d3 = (dact * silu).astype(BF)
        new = (tn(keys, d1), tn(keys, d3), tn(act, target))
        for i in range(3):
            grad[slot, i] = grad[slot, i] + new[i] if add else new[i]

    def attend(b, s, side, gap, begin=False):
        q = q_v[pl.ds(pl.multiple_of(b * rows, rows), rows)]
        k = every[s, side * rows : (side + 1) * rows, :dh]
        v = every[s, side * rows : (side + 1) * rows, dh:]
        diff = lax.broadcasted_iota(jnp.int32, (rows, rows), 0) - lax.broadcasted_iota(
            jnp.int32, (rows, rows), 1
        )
        off = diff + gap * rows
        sc = jnp.where((off >= 0) & (off < WINDOW), nt(q, k), NEG)
        top = jnp.max(sc, axis=1, keepdims=True)
        new = top if begin else jnp.maximum(m_s[b], top)
        p = jnp.exp2((sc - new) * scale)
        lane = sum(p[:, i : i + LANES] for i in range(0, rows, LANES))
        pv = nn(p.astype(BF), v)
        if begin:
            l_s[b] = lane
            acc[b] = pv
        else:
            fade = jnp.exp2((m_s[b] - new) * scale)
            l_s[b] = l_s[b] * fade + lane
            acc[b] = acc[b] * fade + pv
        m_s[b] = new

    def visit(side, s):
        gap = me - s
        if side == 0:
            b = jnp.where(gap >= 0, 0, 1)
            gap = gap + b * n

            @pl.when(gap <= reach)
            def _():
                attend(b, s, 0, gap)
        else:

            @pl.when((gap >= 0) & (gap <= reach))
            def _():
                attend(1, s, 1, gap)

    def visit_all(side):
        def one(s, carry):
            @pl.when(s != me)
            def _():
                visit(side, s)

            return carry

        lax.fori_loop(0, n, one, 0)

    if fine:
        gradients(me, 0, 0, False)
    first_hops(0)
    send_own(1)
    attend(0, me, 0, 0, True)
    attend(1, me, 1, 0, True)

    if n <= reach:
        attend(1, me, 0, n)

    from_mate(0, 1)
    if fine:
        visit(0, me ^ 1)
    near_hops(0)
    for c in evens:
        rate_wait(c)
    if fine:
        for c in evens:
            if c & (c - 1) == 0:
                gradients(me ^ c, c // 2, c // 4, c < 4)
        for c in evens:
            if c & (c - 1) == 0:
                visit(0, me ^ c)
    far_hops(0)
    if fine:
        for c in evens:
            if c & (c - 1):
                gradients(me ^ c, c // 2, 1, True)
        slots = 2 if n > 4 else 1
    else:
        grad[0] = jnp.zeros_like(grad[0])

        def summed(j, carry):
            gradients(2 * j + core, (me // 2) ^ j, 0, True)
            return carry

        lax.fori_loop(0, n // 2, summed, 0)
        slots = 1

    def total(i):
        return grad[0, i] + grad[1, i] if slots == 2 else grad[0, i]

    def g_copy(i):
        return remote(g_out.at[i], g_in.at[i], g_send.at[i], g_recv.at[i], "ctx", me ^ 1)

    def x_copy(i):
        return remote(g_out.at[i], g_in.at[i], x_send.at[i], x_recv.at[i], "ctx", me ^ 1)

    owned = ((0, 1), (2,))

    for own in range(2):

        @pl.when(core == own)
        def _():
            for i in owned[1 - own]:
                g_out[i] = total(i).astype(BF)
                g_copy(i).start()

    def fast_out(b, weights):
        q = q_v[b * rows : (b + 1) * rows]
        h1 = nn(q, weights[0])
        h3 = nn(q, weights[1])
        act = (jax.nn.silu(h1) * h3).astype(BF)
        out = nn(act, weights[2])
        inv = lax.rsqrt(jnp.mean(out * out, axis=1, keepdims=True) + norm_eps)
        normed[...] = out * inv * gain[...]

    chunks = comb.shape[2]
    step = rows // chunks

    def c_copy(b, u):
        return remote(
            comb.at[b, 0, u], comb.at[b, 1, u], c_send.at[b, u], c_recv.at[b, u], "head", mate
        )

    def spot(b, u):
        return pl.ds(b * rows + u * step, step)

    def p_copy(b, u, t):
        return remote(
            tok.at[spot(b, u), pl.ds(t * cols, cols)],
            part_in.at[b, hpair, u],
            p_send.at[b, u, t],
            p_recv.at[b, u, hpair],
            "head",
            t,
        )

    def combine(b):
        both = acc[b] / jnp.sum(l_s[b], axis=1, keepdims=True) + normed[...]
        for u in range(chunks):
            comb[b, 0, u] = both[u * step : (u + 1) * step].astype(BF)
            go(c_copy(b, u))

    def cross(b):
        for u in range(chunks):
            c_copy(b, u).wait_recv()
            for t in range(nh):

                @pl.when(crosses(hme, t))
                def _():
                    tok[spot(b, u), t * cols : (t + 1) * cols] = (
                        nn(comb[b, 0, u], wo[t]) + nn(comb[b, 1, u], wp[t])
                    ).astype(BF)
                    p_copy(b, u, t).start()

        for u in range(chunks):
            res[b, u * step : (u + 1) * step] = nn(comb[b, 0, u], wo[hme]) + nn(
                comb[b, 1, u], wp[hme]
            )

    def close(b):
        for u in range(chunks):
            for pair in range(nh // 2):

                @pl.when(hpair != pair)
                def _():
                    ref = part_in.at[b, pair, u]
                    remote(
                        ref, ref, p_send.at[b, u, 0], p_recv.at[b, u, pair], "head", mate
                    ).wait_recv()
                    here = slice(u * step, (u + 1) * step)
                    res[b, here] = res[b, here] + part_in[b, pair, u].astype(F32)

        q_v[b * rows : (b + 1) * rows] = res[b].astype(BF)
        copy = pltpu.make_async_copy(
            q_v.at[pl.ds(b * rows, rows)], mixed_h.at[b], out_sem.at[3 + b]
        )
        copy.start()
        return copy

    if fine:
        for c in evens:
            if c & (c - 1) == 0:
                from_mate(0, c + 1)
                visit(0, me ^ (c + 1))
        for c in evens:
            if c & (c - 1):
                visit(0, me ^ c)
                from_mate(0, c + 1)
                visit(0, me ^ (c + 1))
    else:
        for c in evens:
            from_mate(0, c + 1)
        visit_all(0)
    fast_out(0, fb)
    for copy in in_wo:
        copy.wait()
    combine(0)

    def ns_steps(mats, count):
        def one(_, carry):
            for i in mats:
                x = grad[0, i]
                xb = x.astype(BF)
                gram = nt(xb, xb)
                gb = gram.astype(BF)
                poly = coeff_b * gram + coeff_c * nn(gb, gb)
                grad[0, i] = coeff_a * x + nn(poly.astype(BF), xb)
            return carry

        lax.fori_loop(0, count, one, 0)

    for own in range(2):

        @pl.when(core == own)
        def _():
            for i in owned[own]:
                g_copy(i).wait_recv()
                g = total(i) + g_in[i].astype(F32)
                grad[0, i] = g * lax.rsqrt(jnp.sum(g * g) + norm_eps)
            ns_steps(owned[own], 1)

    first_hops(1)
    for own in range(2):

        @pl.when(core == own)
        def _():
            ns_steps(owned[own], NS_STEPS - 1)
            for i in owned[own]:
                g_out[i] = grad[0, i].astype(BF)
                x_copy(i).start()

    near_hops(1)
    for t in range(nh):

        @pl.when((hme == t) | crosses(hme, t))
        def _():
            wo_copy(t).wait_recv()

    cross(0)
    from_mate(1, 1)
    if fine:
        visit(1, me ^ 1)
        for c in evens:
            if c & (c - 1) == 0:
                visit(1, me ^ c)
                from_mate(1, c + 1)
                visit(1, me ^ (c + 1))

    outs = (o1_h, o3_h, o2_h)
    for own in range(2):

        @pl.when(core == own)
        def _():
            for i in owned[1 - own]:
                x_copy(i).wait_recv()
                new = f_v[i] - fast_step * g_in[i].astype(F32)
                f_v[i] = new
                fb[i] = new.astype(BF)
            for i in owned[own]:
                new = f_v[i] - fast_step * g_out[i].astype(F32)
                f_v[i] = new
                fb[i] = new.astype(BF)

    writes = [pltpu.make_async_copy(f_v.at[i], outs[i], out_sem.at[i]) for i in range(3)]
    for copy in writes:
        copy.start()
    fast_out(1, fb)
    far_hops(1)
    if fine:
        for c in evens:
            if c & (c - 1):
                visit(1, me ^ c)
                from_mate(1, c + 1)
                visit(1, me ^ (c + 1))
    else:
        for c in evens:
            from_mate(1, c + 1)
        visit_all(1)
    combine(1)
    writes.append(close(0))
    cross(1)
    writes.append(close(1))
    for copy in writes:
        copy.wait()
    for copy in started:
        copy.wait_send()
    for own in range(2):

        @pl.when(core == own)
        def _():
            for i in owned[1 - own]:
                g_copy(i).wait_send()
            for i in owned[own]:
                x_copy(i).wait_send()

    for t in range(nh):

        @pl.when((mate == t) | crosses(mate, t))
        def _():
            wo_copy(t).wait_send()

        @pl.when(crosses(hme, t))
        def _():
            for b in range(2):
                for u in range(chunks):
                    p_copy(b, u, t).wait_send()


def layer(n, nh, rows, flat, w_qkv, w_rate, f1, f3, f2, gain, wo):
    total, width = flat.shape
    blocks = total // rows
    dh, fh = f1.shape
    cols = wo.shape[1] // nh
    chunks = 2
    step = rows // chunks
    dma = pltpu.SemaphoreType.DMA
    return pl.pallas_call(
        functools.partial(layer_kernel, n, nh, rows),
        in_specs=[ANY, ANY, VMEM, ANY, ANY, ANY, VMEM, ANY],
        out_specs=[ANY] * 4,
        out_shape=[jax.ShapeDtypeStruct((blocks, rows, cols), BF)]
        + [jax.ShapeDtypeStruct(f.shape, F32) for f in (f1, f3, f2)],
        scratch_shapes=[
            pltpu.VMEM((total, width), BF),
            pltpu.VMEM((3, width, dh), BF),
            pltpu.VMEM((3, dh, fh), F32),
            pltpu.VMEM((3, dh, fh), BF),
            pltpu.VMEM((nh, dh, cols), BF),
            pltpu.VMEM((nh, dh, cols), BF),
            pltpu.VMEM((total, dh), BF),
            pltpu.VMEM((n, total, 2 * dh), BF),
            pltpu.VMEM((n // 2, 8, rows), F32),
            pltpu.VMEM((2 if n <= 8 else 1, 3, dh, fh), F32),
            pltpu.VMEM((3, dh, fh), BF),
            pltpu.VMEM((3, dh, fh), BF),
            pltpu.VMEM((blocks, rows, 1), F32),
            pltpu.VMEM((blocks, rows, LANES), F32),
            pltpu.VMEM((blocks, rows, dh), F32),
            pltpu.VMEM((rows, dh), F32),
            pltpu.VMEM((blocks, 2, chunks, step, dh), BF),
            pltpu.VMEM((blocks, nh // 2, chunks, step, cols), BF),
            pltpu.VMEM((blocks, rows, cols), F32),
            dma((8 + nh,)),
            dma((2 * blocks, n)),
            dma((2 * blocks, n)),
            dma((n // 2,)),
            dma((n // 2,)),
            dma((3,)),
            dma((3,)),
            dma((3,)),
            dma((3,)),
            dma((nh,)),
            dma((nh,)),
            dma((blocks, chunks)),
            dma((blocks, chunks)),
            dma((blocks, chunks, nh)),
            dma((blocks, chunks, nh // 2)),
            dma((3 + blocks,)),
        ],
        compiler_params=pltpu.CompilerParams(
            vmem_limit_bytes=67_000_000, collective_id=0, has_side_effects=True
        ),
        name="layer",
    )(flat, w_qkv, w_rate, f1, f3, f2, gain, wo)


def shards(tokens, w_qkv, w_rate, w_out, fw_gain, fast_first, fast_third, fast_second):
    blocks, rows, width = tokens.shape
    dh = w_out.shape[1]
    mixed, *current = layer(
        lax.axis_size("ctx"),
        lax.axis_size("head"),
        rows,
        tokens.reshape(blocks * rows, width),
        w_qkv.reshape(width, 3 * dh),
        w_rate.reshape(1, width),
        fast_first[0],
        fast_third[0],
        fast_second[0],
        fw_gain,
        w_out[0],
    )
    return (mixed,) + tuple(f[None] for f in current)


def solution(mesh):
    placed = (
        P(None, "ctx", None),
        P(None, "head", None),
        P(None, "head"),
        P("head", None, None),
        P("head", None),
        P("head", None, None),
        P("head", None, None),
        P("head", None, None),
    )
    return jax.shard_map(
        shards,
        mesh=mesh,
        in_specs=placed,
        out_specs=(
            P(None, "ctx", "head"),
            P("head", None, None),
            P("head", None, None),
            P("head", None, None),
        ),
        check_vma=False,
    )
```

```python
import functools
import math

import jax
import jax.numpy as jnp
from jax import lax
from jax.experimental import pallas as pl
from jax.experimental.pallas import tpu as pltpu
from jax.sharding import PartitionSpec as P

WINDOW = 2048
NS_STEPS = 5

coeff_a = 3.4445
coeff_b = -4.775
coeff_c = 2.0315
fast_step = 0.5
norm_eps = 1e-06
LOG2E = 1.4426950408889634
NEG = -1e30
BF = jnp.bfloat16
F32 = jnp.float32
VMEM = pl.BlockSpec(memory_space=pltpu.VMEM)
ANY = pl.BlockSpec(memory_space=pl.ANY)
HBM = pl.BlockSpec(memory_space=pltpu.HBM)
LANES = 128


def mm(left, right, dims):
    return lax.dot_general(left, right, (dims, ((), ())), preferred_element_type=F32)


def nn(left, right):
    return mm(left, right, ((1,), (0,)))


def nt(left, right):
    return mm(left, right, ((1,), (1,)))


def tn(left, right):
    return mm(left, right, ((0,), (0,)))


def cross_bits(n, sub):
    bits = [1 << i for i in range(1, n.bit_length() - 1)]
    return bits if sub == 0 else bits[::-1]


def remote(src, dst, send, recv, axis, peer):
    return pltpu.make_async_remote_copy(
        src_ref=src,
        dst_ref=dst,
        send_sem=send,
        recv_sem=recv,
        device_id={axis: peer},
        device_id_type=pl.DeviceIdType.MESH,
    )


def layer_kernel(
    n, nh, rows,
    tok_h, w_h, wr_h, f1_h, f3_h, f2_h, gain_h, wo_h,
    mixed_h, o1_h, o3_h, o2_h,
    tok, w, wr, gain, f_v, fb, wo, wp, q_v, every, rates,
    grad, g_out, g_in,
    m_s, l_s, acc, normed, comb, part_in, res,
    load, k_send, k_recv, s_send, s_recv, g_send, g_recv, x_send, x_recv,
    w_send, w_recv, c_send, c_recv, p_send, p_recv, out_sem,
):
    me = lax.axis_index("ctx")
    hme = lax.axis_index("head")
    dh = q_v.shape[1]
    cols = wo.shape[2]
    reach = WINDOW // rows
    scale = dh ** (-0.5) * LOG2E
    core = lax.rem(me, 2)
    fine = n <= 8
    evens = sorted(range(2, n, 2), key=lambda c: (bin(c).count("1"), c))
    hpair = hme // 2
    hodd = lax.rem(hme, 2)
    mate = hme + 1 - 2 * hodd

    def fetch(i, src, dst):
        copy = pltpu.make_async_copy(src, dst, load.at[i])
        copy.start()
        return copy

    first, second = pl.ds(0, rows), pl.ds(rows, rows)
    in_tok0 = fetch(0, tok_h.at[first], tok.at[first])
    in_k = fetch(1, w_h.at[:, pl.ds(dh, dh)], w.at[1])

    barrier = pltpu.get_barrier_semaphore()
    peers = [1] + evens
    for c in peers:
        pl.semaphore_signal(
            barrier, inc=1, device_id={"ctx": me ^ c}, device_id_type=pl.DeviceIdType.MESH
        )
    for r in range(1, nh):
        pl.semaphore_signal(
            barrier,
            inc=1,
            device_id={"head": lax.rem(hme + r, nh)},
            device_id_type=pl.DeviceIdType.MESH,
        )

    started = []

    def go(make):
        make().start()
        started.append(make)

    half = rows // 2

    def piece(p, c):
        b, kv, sub = p // 4, p // 2 % 2, p % 2
        return every.at[me ^ c, kv, pl.ds(b * rows + sub * half, half)]

    def pieces(b):
        return [(4 * b + 2 * kv + sub, sub) for kv in range(2) for sub in range(2)]

    def kv_copy(p, c, bit):
        ref = piece(p, c)
        return remote(ref, ref, k_send.at[p, c | bit], k_recv.at[p, c | bit], "ctx", me ^ bit)

    def kv_wait(p, c):
        ref = piece(p, c)
        remote(ref, ref, k_send.at[p, c], k_recv.at[p, c], "ctx", me ^ (c & -c)).wait_recv()

    def pass_on(p, c):
        order = cross_bits(n, p % 2)
        last = max(i for i, bit in enumerate(order) if c & bit)
        for bit in order[last + 1 :]:
            go(functools.partial(kv_copy, p, c, bit))
        go(functools.partial(kv_copy, p, c, 1))

    def send_own(b, kv, turns):
        for turn in turns:
            for sub in range(2):
                bits = cross_bits(n, sub)
                go(functools.partial(kv_copy, 4 * b + 2 * kv + sub, 0, bits[turn]))
        if 0 in turns:
            for sub in range(2):
                go(functools.partial(kv_copy, 4 * b + 2 * kv + sub, 0, 1))

    later_turns = range(1, len(cross_bits(n, 0)))

    def hops(b, far, first):
        for c in evens:
            for p, sub in pieces(b):
                if far == (c & (c - 1) != 0) and (far or first == (c == cross_bits(n, sub)[0])):
                    kv_wait(p, c)
                    pass_on(p, c)

    def first_hops(b):
        hops(b, False, True)

    def near_hops(b):
        hops(b, False, False)

    def far_hops(b):
        hops(b, True, False)

    def from_mate(b, c):
        for p, _ in pieces(b):
            kv_wait(p, c)

    in_tok0.wait()
    in_k.wait()
    in_v = fetch(2, w_h.at[:, pl.ds(2 * dh, dh)], w.at[2])
    in_wr = fetch(8 + nh, wr_h, wr)
    in_gain = fetch(9 + nh, gain_h, gain)
    every[me, 0, :rows] = nn(tok[:rows], w[1]).astype(BF)
    pl.semaphore_wait(barrier, len(peers) + nh - 1)
    send_own(0, 0, (0,))
    in_v.wait()
    in_tok1 = fetch(3, tok_h.at[second], tok.at[second])
    in_q = fetch(4, w_h.at[:, pl.ds(0, dh)], w.at[0])
    in_f = [fetch(5 + i, f, f_v.at[i]) for i, f in enumerate((f1_h, f3_h, f2_h))]
    in_wo = [
        fetch(8 + t, wo_h.at[:, pl.ds(t * cols, cols)], wo.at[t]) for t in range(nh)
    ]
    every[me, 1, :rows] = nn(tok[:rows], w[2]).astype(BF)
    send_own(0, 1, (0,))
    for kv in range(2):
        send_own(0, kv, later_turns)

    def rate_copy(c):
        i = c // 2
        return remote(rates.at[0], rates.at[i], s_send.at[i], s_recv.at[i], "ctx", me ^ c)

    in_wr.wait()
    logit = nt(jnp.broadcast_to(wr[...], (8, wr.shape[1])), tok[:rows])
    rates[0] = jnp.maximum(logit, 0.0) + jnp.log1p(jnp.exp(-jnp.abs(logit)))
    for c in evens:
        go(functools.partial(rate_copy, c))

    def crosses(h, t):
        odd = lax.rem(h, 2)
        up = (odd == 1) & (t // 2 > h // 2)
        down = (odd == 0) & (t // 2 < h // 2)
        return up | down

    share = pl.ds(pl.multiple_of(core * (dh // 2), dh // 2), dh // 2)

    def wo_copy(t):
        return remote(
            wo_h.at[share, pl.ds(t * cols, cols)],
            wp.at[t, share],
            w_send.at[0, t],
            w_recv.at[0, t],
            "head",
            mate,
        )

    def wo_pass(t):
        ref = wp.at[t, share]
        return remote(ref, ref, w_send.at[1, t], w_recv.at[1, t], "ctx", me ^ 1)

    def wo_gets(t):
        return (hme == t) | crosses(hme, t)

    for t in range(nh):

        @pl.when((mate == t) | crosses(mate, t))
        def _():
            wo_copy(t).start()

    in_tok1.wait()
    every[me, 0, rows:] = nn(tok[rows:], w[1]).astype(BF)
    every[me, 1, rows:] = nn(tok[rows:], w[2]).astype(BF)
    in_q.wait()
    in_gain.wait()
    q_v[...] = nn(tok[...], w[0]).astype(BF)
    for i in range(3):
        in_f[i].wait()
        fb[i] = f_v[i].astype(BF)

    def gradients(s, at, slot, add, close_sum=False):
        keys = every[s, 0, :rows]
        vals = every[s, 1, :rows]
        rate = jnp.transpose(rates[at])[:, :1]
        target = (-rate * vals.astype(F32)).astype(BF)
        h1 = nn(keys, fb[0])
        h3 = nn(keys, fb[1])
        sig = jax.nn.sigmoid(h1)
        silu = h1 * sig
        act = (silu * h3).astype(BF)
        dact = nt(target, fb[2])
        d1 = (dact * h3 * (sig * (1.0 + h1 * (1.0 - sig)))).astype(BF)
        d3 = (dact * silu).astype(BF)
        new = (tn(keys, d1), tn(keys, d3), tn(act, target))
        for i in range(3):
            if close_sum:
                grad[0, i] = grad[0, i] + (grad[1, i] + new[i])
            else:
                grad[slot, i] = grad[slot, i] + new[i] if add else new[i]

    def attend(b, sources, side, gap=None, begin=False, hide=None):
        q = q_v[pl.ds(pl.multiple_of(b * rows, rows), rows)]
        span = pl.ds(side * rows, rows)
        scores = [nt(q, every[s, 0, span]) for s in sources]
        if gap is not None:
            off = (
                lax.broadcasted_iota(jnp.int32, (rows, rows), 0)
                - lax.broadcasted_iota(jnp.int32, (rows, rows), 1)
                + gap * rows
            )
            scores = [jnp.where((off >= 0) & (off < WINDOW), sc, NEG) for sc in scores]
        if hide is not None:
            scores = [sc + bias for sc, bias in zip(scores, hide)]
        top = functools.reduce(jnp.maximum, scores)
        new = jnp.max(top, axis=1, keepdims=True)
        if not begin:
            new = jnp.maximum(m_s[b], new)
        probs = [jnp.exp2((sc - new) * scale) for sc in scores]
        lane = sum(p[:, i : i + LANES] for p in probs for i in range(0, rows, LANES))
        pv = sum(nn(p.astype(BF), every[s, 1, span]) for p, s in zip(probs, sources))
        if begin:
            l_s[b] = lane
            acc[b] = pv
        else:
            fade = jnp.exp2((m_s[b] - new) * scale)
            l_s[b] = l_s[b] * fade + lane
            acc[b] = acc[b] * fade + pv
        m_s[b] = new

    def visit(c):
        sources = [me ^ c] if c == 1 else [me ^ c, me ^ c ^ 1]
        attend(jnp.where(me > me ^ c, 0, 1), sources, 0)

    def visit_before(single, chips):
        sources = [me ^ c for c in single] + [me ^ c ^ i for c in chips for i in range(2)]
        attend(1, sources, 1, hide=[jnp.where(me > s, 0.0, NEG) for s in sources])

    def visit_all(side):
        def one(s, carry):
            gap = me - s
            b = jnp.where(gap >= 0, side, 1)
            gap = gap + (b - side) * n

            @pl.when((s != me) & (gap >= 0) & (gap <= reach))
            def _():
                attend(b, [s], side, gap)

            return carry

        lax.fori_loop(0, n, one, 0)

    def fast_out(b, weights):
        q = q_v[b * rows : (b + 1) * rows]
        h1 = nn(q, weights[0])
        h3 = nn(q, weights[1])
        act = (jax.nn.silu(h1) * h3).astype(BF)
        out = nn(act, weights[2])
        inv = lax.rsqrt(jnp.mean(out * out, axis=1, keepdims=True) + norm_eps)
        normed[...] = out * inv * gain[...]

    if fine:
        gradients(me, 0, 0, False)
    fast_out(0, fb)
    attend(0, [me], 0, 0, True)
    first_hops(0)
    for turns in ((0,), later_turns):
        for kv in range(2):
            send_own(1, kv, turns)
    attend(1, [me], 1, 0, True)
    if n <= reach:
        attend(1, [me], 0, n)
    from_mate(0, 1)
    if fine:
        visit(1)
    near_hops(0)
    for c in evens:
        rate_copy(c).wait_recv()
    if fine:
        for c in evens:
            if c & (c - 1) == 0:
                gradients(me ^ c, c // 2, c // 4, c < 4)
        for c in evens:
            if c & (c - 1) == 0:
                from_mate(0, c + 1)
                visit(c)
    far_hops(0)
    if fine:
        for c in evens:
            if c & (c - 1):
                gradients(me ^ c, c // 2, 1, True, True)
    else:
        grad[0] = jnp.zeros_like(grad[0])

        def summed(j, carry):
            gradients(2 * j + core, (me // 2) ^ j, 0, True)
            return carry

        lax.fori_loop(0, n // 2, summed, 0)

    def g_copy(i):
        return remote(g_out.at[i], g_in.at[i], g_send.at[i], g_recv.at[i], "ctx", me ^ 1)

    def x_copy(i):
        return remote(g_out.at[i], g_in.at[i], x_send.at[i], x_recv.at[i], "ctx", me ^ 1)

    owned = ((0, 1), (2,))

    for own in range(2):

        @pl.when(core == own)
        def _():
            for i in owned[1 - own]:
                g_out[i] = grad[0, i].astype(BF)
                g_copy(i).start()

    chunks = comb.shape[2]
    step = rows // chunks

    def c_copy(b, u):
        return remote(
            comb.at[b, 0, u], comb.at[b, 1, u], c_send.at[b, u], c_recv.at[b, u], "head", mate
        )

    def spot(b, u):
        return pl.ds(b * rows + u * step, step)

    def p_copy(b, u, t):
        return remote(
            tok.at[spot(b, u), pl.ds(t * cols, cols)],
            part_in.at[b, hpair, u],
            p_send.at[b, u, t],
            p_recv.at[b, u, hpair],
            "head",
            t,
        )

    def combine(b):
        both = acc[b] / jnp.sum(l_s[b], axis=1, keepdims=True) + normed[...]
        for u in range(chunks):
            comb[b, 0, u] = both[u * step : (u + 1) * step].astype(BF)
            go(functools.partial(c_copy, b, u))

    def cross(b):
        for u in range(chunks):
            c_copy(b, u).wait_recv()
            for t in range(nh):

                @pl.when(crosses(hme, t))
                def _():
                    tok[spot(b, u), t * cols : (t + 1) * cols] = (
                        nn(comb[b, 0, u], wo[t]) + nn(comb[b, 1, u], wp[t])
                    ).astype(BF)
                    p_copy(b, u, t).start()

        for u in range(chunks):
            res[b, u * step : (u + 1) * step] = nn(comb[b, 0, u], wo[hme]) + nn(
                comb[b, 1, u], wp[hme]
            )

    def close(b):
        for u in range(chunks):
            for pair in range(nh // 2):

                @pl.when(hpair != pair)
                def _():
                    ref = part_in.at[b, pair, u]
                    remote(
                        ref, ref, p_send.at[b, u, 0], p_recv.at[b, u, pair], "head", mate
                    ).wait_recv()
                    here = slice(u * step, (u + 1) * step)
                    res[b, here] = res[b, here] + part_in[b, pair, u].astype(F32)

        q_v[b * rows : (b + 1) * rows] = res[b].astype(BF)
        copy = pltpu.make_async_copy(
            q_v.at[pl.ds(b * rows, rows)], mixed_h.at[b], out_sem.at[3 + b]
        )
        copy.start()
        return copy

    for t in range(nh):

        @pl.when(wo_gets(t))
        def _():
            wo_copy(t).wait_recv()
            wo_pass(t).start()

    if fine:
        for c in evens:
            if c & (c - 1):
                from_mate(0, c + 1)
                visit(c)
    else:
        for c in evens:
            from_mate(0, c + 1)
        visit_all(0)
    combine(0)

    def ns_steps(mats, count, norms=None):
        def one(_, carry):
            for at, i in enumerate(mats):
                x = grad[0, i] if norms is None else grad[0, i] * norms[at]
                xb = x.astype(BF)
                gram = nt(xb, xb)
                gb = gram.astype(BF)
                poly = coeff_b * gram + coeff_c * nn(gb, gb)
                grad[0, i] = coeff_a * x + nn(poly.astype(BF), xb)
            return carry

        if count == 1:
            one(0, 0)
        else:
            lax.fori_loop(0, count, one, 0)

    for own in range(2):

        @pl.when(core == own)
        def _():
            norms = []
            for i in owned[own]:
                g_copy(i).wait_recv()
                g = grad[0, i] + g_in[i].astype(F32)
                grad[0, i] = g
                norms.append(lax.rsqrt(jnp.sum(g * g) + norm_eps))
            ns_steps(owned[own], 1, norms)

    first_hops(1)
    for own in range(2):

        @pl.when(core == own)
        def _():
            ns_steps(owned[own], 2)

    for t in range(nh):

        @pl.when(wo_gets(t))
        def _():
            wo_pass(t).wait_recv()

    for copy in in_wo:
        copy.wait()
    cross(0)
    near_hops(1)
    for own in range(2):

        @pl.when(core == own)
        def _():
            ns_steps(owned[own], NS_STEPS - 4)

    far_hops(1)
    for own in range(2):

        @pl.when(core == own)
        def _():
            ns_steps(owned[own], 1)
            for i in owned[own]:
                g_out[i] = grad[0, i].astype(BF)
                x_copy(i).start()

    from_mate(1, 1)
    if fine:
        for far in (False, True):
            chips = [c for c in evens if far == (c & (c - 1) != 0)]
            for c in chips:
                from_mate(1, c + 1)
            visit_before([] if far else [1], chips)
    else:
        for c in evens:
            from_mate(1, c + 1)
        visit_all(1)

    def stepped(own, i):
        moved = g_out[i] if i in owned[own] else g_in[i]
        return f_v[i] - fast_step * moved.astype(F32)

    for own in range(2):

        @pl.when(core == own)
        def _():
            for i in owned[1 - own]:
                x_copy(i).wait_recv()
            for i in range(3):
                fb[i] = stepped(own, i).astype(BF)

    fast_out(1, fb)
    combine(1)
    for own in range(2):

        @pl.when(core == own)
        def _():
            for i in range(3):
                f_v[i] = stepped(own, i)

    outs = (o1_h, o3_h, o2_h)
    writes = [pltpu.make_async_copy(f_v.at[i], outs[i], out_sem.at[i]) for i in range(3)]
    for copy in writes:
        copy.start()
    writes.append(close(0))
    cross(1)
    writes.append(close(1))
    for copy in writes:
        copy.wait()
    for make in started:
        make().wait_send()
    for own in range(2):

        @pl.when(core == own)
        def _():
            for i in owned[1 - own]:
                g_copy(i).wait_send()
            for i in owned[own]:
                x_copy(i).wait_send()

    for t in range(nh):

        @pl.when((mate == t) | crosses(mate, t))
        def _():
            wo_copy(t).wait_send()

        @pl.when(wo_gets(t))
        def _():
            wo_pass(t).wait_send()

        @pl.when(crosses(hme, t))
        def _():
            for b in range(2):
                for u in range(chunks):
                    p_copy(b, u, t).wait_send()


def layer(n, nh, rows, flat, w_qkv, w_rate, f1, f3, f2, gain, wo):
    total, width = flat.shape
    blocks = total // rows
    dh, fh = f1.shape
    cols = wo.shape[1] // nh
    chunks = 4
    step = rows // chunks
    dma = pltpu.SemaphoreType.DMA
    buffers = [
        pltpu.VMEM((total, width), BF),
        pltpu.VMEM((3, width, dh), BF),
        pltpu.VMEM((1, width), BF),
        pltpu.VMEM((1, dh), F32),
        pltpu.VMEM((3, dh, fh), F32),
        pltpu.VMEM((3, dh, fh), BF),
        pltpu.VMEM((nh, dh, cols), BF),
        pltpu.VMEM((nh, dh, cols), BF),
        pltpu.VMEM((total, dh), BF),
        pltpu.VMEM((n, 2, total, dh), BF),
        pltpu.VMEM((n // 2, 8, rows), F32),
        pltpu.VMEM((2 if n <= 8 else 1, 3, dh, fh), F32),
        pltpu.VMEM((3, dh, fh), BF),
        pltpu.VMEM((3, dh, fh), BF),
        pltpu.VMEM((blocks, rows, 1), F32),
        pltpu.VMEM((blocks, rows, LANES), F32),
        pltpu.VMEM((blocks, rows, dh), F32),
        pltpu.VMEM((rows, dh), F32),
        pltpu.VMEM((blocks, 2, chunks, step, dh), BF),
        pltpu.VMEM((blocks, nh // 2, chunks, step, cols), BF),
        pltpu.VMEM((blocks, rows, cols), F32),
    ]
    need = sum(math.prod(b.shape) * jnp.dtype(b.dtype).itemsize for b in buffers)
    return pl.pallas_call(
        functools.partial(layer_kernel, n, nh, rows),
        in_specs=[HBM] * 8,
        out_specs=[ANY] * 4,
        out_shape=[jax.ShapeDtypeStruct((blocks, rows, cols), BF)]
        + [jax.ShapeDtypeStruct(f.shape, F32) for f in (f1, f3, f2)],
        scratch_shapes=[
            *buffers,
            dma((10 + nh,)),
            dma((4 * blocks, n)),
            dma((4 * blocks, n)),
            dma((n // 2,)),
            dma((n // 2,)),
            dma((3,)),
            dma((3,)),
            dma((3,)),
            dma((3,)),
            dma((2, nh)),
            dma((2, nh)),
            dma((blocks, chunks)),
            dma((blocks, chunks)),
            dma((blocks, chunks, nh)),
            dma((blocks, chunks, nh // 2)),
            dma((3 + blocks,)),
        ],
        compiler_params=pltpu.CompilerParams(
            vmem_limit_bytes=min(67_000_000, need + 6_000_000), collective_id=0, has_side_effects=True
        ),
        name="layer",
    )(
        *(
            pltpu.with_memory_space_constraint(x, pltpu.HBM)
            for x in (flat, w_qkv, w_rate, f1, f3, f2, gain, wo)
        )
    )


def shards(tokens, w_qkv, w_rate, w_out, fw_gain, fast_first, fast_third, fast_second):
    blocks, rows, width = tokens.shape
    dh = w_out.shape[1]
    mixed, *current = layer(
        lax.axis_size("ctx"),
        lax.axis_size("head"),
        rows,
        tokens.reshape(blocks * rows, width),
        w_qkv.reshape(width, 3 * dh),
        w_rate.reshape(1, width),
        fast_first[0],
        fast_third[0],
        fast_second[0],
        fw_gain,
        w_out[0],
    )
    return (mixed,) + tuple(f[None] for f in current)


def solution(mesh):
    placed = (
        P(None, "ctx", None),
        P(None, "head", None),
        P(None, "head"),
        P("head", None, None),
        P("head", None),
        P("head", None, None),
        P("head", None, None),
        P("head", None, None),
    )
    return jax.shard_map(
        shards,
        mesh=mesh,
        in_specs=placed,
        out_specs=(
            P(None, "ctx", "head"),
            P("head", None, None),
            P("head", None, None),
            P("head", None, None),
        ),
        check_vma=False,
    )
```

```python
import functools
import math

import jax
import jax.numpy as jnp
from jax import lax
from jax.experimental import pallas as pl
from jax.experimental.pallas import tpu as pltpu
from jax.sharding import PartitionSpec as P

WINDOW = 2048
NS_STEPS = 5

coeff_a = 3.4445
coeff_b = -4.775
coeff_c = 2.0315
fast_step = 0.5
norm_eps = 1e-06
LOG2E = 1.4426950408889634
NEG = -1e30
BF = jnp.bfloat16
F32 = jnp.float32
VMEM = pl.BlockSpec(memory_space=pltpu.VMEM)
ANY = pl.BlockSpec(memory_space=pl.ANY)
HBM = pl.BlockSpec(memory_space=pltpu.HBM)
LANES = 128


def mm(left, right, dims):
    return lax.dot_general(left, right, (dims, ((), ())), preferred_element_type=F32)


def nn(left, right):
    return mm(left, right, ((1,), (0,)))


def nt(left, right):
    return mm(left, right, ((1,), (1,)))


def tn(left, right):
    return mm(left, right, ((0,), (0,)))


def cross_bits(n, sub):
    bits = [1 << i for i in range(1, n.bit_length() - 1)]
    return bits if sub == 0 else bits[::-1]


def arrivals(n):
    slots = {}
    for b in range(2):
        for c in range(1, n):
            for sub in range(2):
                for kv in range(2):
                    if c % 2:
                        key = (b, c, None, None)
                    elif c == cross_bits(n, sub)[0]:
                        key = (b, c, sub, kv)
                    else:
                        key = (b, c, sub, None)
                    slots.setdefault(key, len(slots))
    return slots


def remote(src, dst, send, recv, axis, peer):
    return pltpu.make_async_remote_copy(
        src_ref=src,
        dst_ref=dst,
        send_sem=send,
        recv_sem=recv,
        device_id={axis: peer},
        device_id_type=pl.DeviceIdType.MESH,
    )


def layer_kernel(
    n, nh, rows,
    tok_h, w_h, wr_h, f1_h, f3_h, f2_h, gain_h, wo_h,
    mixed_h, o1_h, o3_h, o2_h,
    tok, w, wr, gain, f_v, fb, wo, wp, q_v, every, rates,
    grad, g_out, g_in,
    m_s, l_s, acc, normed, comb, part_in, res,
    load, k_send, k_recv, s_send, s_recv, e_send, e_recv,
    w_send, w_recv, c_send, c_recv, p_send, p_recv, out_sem,
):
    me = lax.axis_index("ctx")
    hme = lax.axis_index("head")
    dh = q_v.shape[1]
    cols = wo.shape[2]
    reach = WINDOW // rows
    scale = dh ** (-0.5) * LOG2E
    core = lax.rem(me, 2)
    fine = n <= 8
    evens = sorted(range(2, n, 2), key=lambda c: (bin(c).count("1"), c))
    hpair = hme // 2
    hodd = lax.rem(hme, 2)
    mate = hme + 1 - 2 * hodd

    def fetch(i, src, dst):
        copy = pltpu.make_async_copy(src, dst, load.at[i])
        copy.start()
        return copy

    first, second = pl.ds(0, rows), pl.ds(rows, rows)
    in_tok0 = fetch(0, tok_h.at[first], tok.at[first])
    in_k = fetch(1, w_h.at[:, pl.ds(dh, dh)], w.at[1])

    barrier = pltpu.get_barrier_semaphore()
    peers = [1] + evens
    for c in peers:
        pl.semaphore_signal(
            barrier, inc=1, device_id={"ctx": me ^ c}, device_id_type=pl.DeviceIdType.MESH
        )
    for r in range(1, nh):
        pl.semaphore_signal(
            barrier,
            inc=1,
            device_id={"head": lax.rem(hme + r, nh)},
            device_id_type=pl.DeviceIdType.MESH,
        )

    half = rows // 2
    slots = arrivals(n)

    def piece(b, c, sub, kv):
        span = pl.ds(b * rows, rows) if sub is None else pl.ds(b * rows + sub * half, half)
        return every.at[me ^ c, slice(None) if kv is None else kv, span]

    def slot(b, c, sub, kv):
        for key in ((b, c, sub, kv), (b, c, sub, None), (b, c, None, None)):
            if key in slots:
                return slots[key]

    def kv_copy(b, c, sub, kv, bit):
        ref = piece(b, c, sub, kv)
        return remote(
            ref, ref, k_send.at[b, sub], k_recv.at[slot(b, c | bit, sub, kv)], "ctx", me ^ bit
        )

    def kv_wait(b, c, sub=None, kv=None):
        ref = piece(b, c, sub, kv)
        at = k_recv.at[slot(b, c, sub, kv)]
        remote(ref, ref, k_send.at[0, 0], at, "ctx", me ^ (c & -c)).wait_recv()

    def pass_on(b, c, sub, kv):
        order = cross_bits(n, sub)
        last = max(i for i, bit in enumerate(order) if c & bit)
        for bit in order[last + 1 :] + [1]:
            kv_copy(b, c, sub, kv, bit).start()

    def send_own(b, kv, turns):
        for turn in turns:
            for sub in range(2):
                kv_copy(b, 0, sub, kv, cross_bits(n, sub)[turn]).start()
        if 0 in turns:
            for sub in range(2):
                kv_copy(b, 0, sub, kv, 1).start()

    def kv_sent():
        for b in range(2):
            for sub in range(2):
                ref = every.at[pl.ds(0, n - 1), :, pl.ds(0, half)]
                remote(
                    ref, ref, k_send.at[b, sub], k_recv.at[0], "ctx", me ^ 1
                ).wait_send()

    later_turns = range(1, len(cross_bits(n, 0)))

    def hops(b, far, first):
        for c in evens:
            for kv in range(2) if first else (None,):
                for sub in range(2):
                    near = c == cross_bits(n, sub)[0]
                    if far == (c & (c - 1) != 0) and (far or first == near):
                        kv_wait(b, c, sub, kv)
                        pass_on(b, c, sub, kv)

    def first_hops(b):
        hops(b, False, True)

    def near_hops(b):
        hops(b, False, False)

    def far_hops(b):
        hops(b, True, False)

    def from_mate(b, c):
        kv_wait(b, c)

    in_tok0.wait()
    in_k.wait()
    in_v = fetch(2, w_h.at[:, pl.ds(2 * dh, dh)], w.at[2])
    in_wr = fetch(7, wr_h, wr)
    in_gain = fetch(8, gain_h, gain)
    every[me, 0, :rows] = nn(tok[:rows], w[1]).astype(BF)
    pl.semaphore_wait(barrier, len(peers) + nh - 1)
    send_own(0, 0, (0,))
    in_v.wait()
    in_tok1 = fetch(3, tok_h.at[second], tok.at[second])
    in_q = fetch(4, w_h.at[:, pl.ds(0, dh)], w.at[0])
    for i, f in enumerate((f1_h, f3_h, f2_h)):
        fetch(5, f, f_v.at[i])
    in_f = pltpu.make_async_copy(f_v, f_v, load.at[5])
    for t in range(nh):
        fetch(6, wo_h.at[:, pl.ds(t * cols, cols)], wo.at[t])
    in_wo = pltpu.make_async_copy(wo, wo, load.at[6])
    every[me, 1, :rows] = nn(tok[:rows], w[2]).astype(BF)
    send_own(0, 1, (0,))
    send_own(0, None, later_turns)

    def rate_copy(c):
        i = c // 2
        return remote(rates.at[0], rates.at[i], s_send, s_recv, "ctx", me ^ c)

    in_wr.wait()
    logit = nt(jnp.broadcast_to(wr[...], (8, wr.shape[1])), tok[:rows])
    rates[0] = jnp.maximum(logit, 0.0) + jnp.log1p(jnp.exp(-jnp.abs(logit)))
    for c in evens:
        rate_copy(c).start()

    others = rates.at[pl.ds(1, n // 2 - 1)]
    all_rates = remote(others, others, s_send, s_recv, "ctx", me ^ 1)

    def crosses(h, t):
        odd = lax.rem(h, 2)
        up = (odd == 1) & (t // 2 > h // 2)
        down = (odd == 0) & (t // 2 < h // 2)
        return up | down

    share = pl.ds(pl.multiple_of(core * (dh // 2), dh // 2), dh // 2)

    def wo_copy(t):
        return remote(
            wo_h.at[share, pl.ds(t * cols, cols)],
            wp.at[t, share],
            w_send.at[0, t],
            w_recv.at[0, t],
            "head",
            mate,
        )

    def wo_pass(t):
        ref = wp.at[t, share]
        return remote(ref, ref, w_send.at[1, t], w_recv.at[1, t], "ctx", me ^ 1)

    def wo_gets(t):
        return (hme == t) | crosses(hme, t)

    for t in range(nh):

        @pl.when((mate == t) | crosses(mate, t))
        def _():
            wo_copy(t).start()

    in_tok1.wait()
    every[me, 0, rows:] = nn(tok[rows:], w[1]).astype(BF)
    every[me, 1, rows:] = nn(tok[rows:], w[2]).astype(BF)
    in_q.wait()
    in_gain.wait()
    q_v[...] = nn(tok[...], w[0]).astype(BF)
    in_f.wait()
    for i in range(3):
        fb[i] = f_v[i].astype(BF)

    def gradients(s, at, slot, add, close_sum=False):
        keys = every[s, 0, :rows]
        vals = every[s, 1, :rows]
        rate = jnp.transpose(rates[at])[:, :1]
        target = (-rate * vals.astype(F32)).astype(BF)
        h1 = nn(keys, fb[0])
        h3 = nn(keys, fb[1])
        sig = jax.nn.sigmoid(h1)
        silu = h1 * sig
        act = (silu * h3).astype(BF)
        dact = nt(target, fb[2])
        d1 = (dact * h3 * (sig * (1.0 + h1 * (1.0 - sig)))).astype(BF)
        d3 = (dact * silu).astype(BF)
        new = (tn(keys, d1), tn(keys, d3), tn(act, target))
        for i in range(3):
            if close_sum:
                grad[0, i] = grad[0, i] + (grad[1, i] + new[i])
            else:
                grad[slot, i] = grad[slot, i] + new[i] if add else new[i]

    def attend(b, sources, side, gap=None, begin=False, hide=None):
        q = q_v[pl.ds(pl.multiple_of(b * rows, rows), rows)]
        span = pl.ds(side * rows, rows)
        scores = [nt(q, every[s, 0, span]) for s in sources]
        if gap is not None:
            off = (
                lax.broadcasted_iota(jnp.int32, (rows, rows), 0)
                - lax.broadcasted_iota(jnp.int32, (rows, rows), 1)
                + gap * rows
            )
            scores = [jnp.where((off >= 0) & (off < WINDOW), sc, NEG) for sc in scores]
        if hide is not None:
            scores = [sc + bias for sc, bias in zip(scores, hide)]
        top = functools.reduce(jnp.maximum, scores)
        new = jnp.max(top, axis=1, keepdims=True)
        if not begin:
            new = jnp.maximum(m_s[b], new)
        probs = [jnp.exp2((sc - new) * scale) for sc in scores]
        lane = sum(p[:, i : i + LANES] for p in probs for i in range(0, rows, LANES))
        pv = sum(nn(p.astype(BF), every[s, 1, span]) for p, s in zip(probs, sources))
        if begin:
            l_s[b] = lane
            acc[b] = pv
        else:
            fade = jnp.exp2((m_s[b] - new) * scale)
            l_s[b] = l_s[b] * fade + lane
            acc[b] = acc[b] * fade + pv
        m_s[b] = new

    def visit(c):
        sources = [me ^ c] if c == 1 else [me ^ c, me ^ c ^ 1]
        attend(jnp.where(me > me ^ c, 0, 1), sources, 0)

    def visit_before(single, chips):
        sources = [me ^ c for c in single] + [me ^ c ^ i for c in chips for i in range(2)]
        attend(1, sources, 1, hide=[jnp.where(me > s, 0.0, NEG) for s in sources])

    def visit_all(side):
        def one(s, carry):
            gap = me - s
            b = jnp.where(gap >= 0, side, 1)
            gap = gap + (b - side) * n

            @pl.when((s != me) & (gap >= 0) & (gap <= reach))
            def _():
                attend(b, [s], side, gap)

            return carry

        lax.fori_loop(0, n, one, 0)

    def fast_out(b, weights):
        q = q_v[b * rows : (b + 1) * rows]
        h1 = nn(q, weights[0])
        h3 = nn(q, weights[1])
        act = (jax.nn.silu(h1) * h3).astype(BF)
        out = nn(act, weights[2])
        inv = lax.rsqrt(jnp.mean(out * out, axis=1, keepdims=True) + norm_eps)
        normed[...] = out * inv * gain[...]

    if fine:
        gradients(me, 0, 0, False)
    fast_out(0, fb)
    attend(0, [me], 0, 0, True)
    first_hops(0)
    for kv in range(2):
        send_own(1, kv, (0,))
    send_own(1, None, later_turns)
    attend(1, [me], 1, 0, True)
    if n <= reach:
        attend(1, [me], 0, n)
    from_mate(0, 1)
    if fine:
        visit(1)
    near_hops(0)
    all_rates.wait_recv()
    if fine:
        for c in evens:
            if c & (c - 1) == 0:
                gradients(me ^ c, c // 2, c // 4, c < 4)
        for c in evens:
            if c & (c - 1) == 0:
                from_mate(0, c + 1)
                visit(c)
    far_hops(0)
    if fine:
        for c in evens:
            if c & (c - 1):
                gradients(me ^ c, c // 2, 1, True, True)
    else:
        grad[0] = jnp.zeros_like(grad[0])

        def summed(j, carry):
            gradients(2 * j + core, (me // 2) ^ j, 0, True)
            return carry

        lax.fori_loop(0, n // 2, summed, 0)

    def g_copy(i):
        return remote(g_out.at[i], g_in.at[i], e_send.at[i], e_recv.at[i], "ctx", me ^ 1)

    def x_copy(i):
        return remote(g_out.at[i], g_in.at[i], e_send.at[i], e_recv.at[i], "ctx", me ^ 1)

    owned = ((0, 1), (2,))

    for own in range(2):

        @pl.when(core == own)
        def _():
            for i in owned[1 - own]:
                g_out[i] = grad[0, i].astype(BF)
                g_copy(i).start()

    chunks = comb.shape[2]
    pairs = nh // 2
    step = rows // chunks

    def c_copy(b, u):
        return remote(
            comb.at[b, 0, u], comb.at[b, 1, u], c_send.at[b], c_recv.at[b, u], "head", mate
        )

    def spot(b, u):
        return pl.ds(b * rows + u * step, step)

    def p_copy(b, u, t):
        return remote(
            tok.at[spot(b, u), pl.ds(t * cols, cols)],
            part_in.at[b, lax.rem(hpair - t // 2 + pairs, pairs) - 1, u],
            p_send.at[b, t],
            p_recv.at[b, u, lax.rem(hpair - t // 2 + pairs, pairs) - 1],
            "head",
            t,
        )

    def combine(b):
        both = acc[b] / jnp.sum(l_s[b], axis=1, keepdims=True) + normed[...]
        for u in range(chunks):
            comb[b, 0, u] = both[u * step : (u + 1) * step].astype(BF)
            c_copy(b, u).start()

    def cross(b):
        for u in range(chunks):
            c_copy(b, u).wait_recv()
            for t in range(nh):

                @pl.when(crosses(hme, t))
                def _():
                    tok[spot(b, u), t * cols : (t + 1) * cols] = (
                        nn(comb[b, 0, u], wo[t]) + nn(comb[b, 1, u], wp[t])
                    ).astype(BF)
                    p_copy(b, u, t).start()

        for u in range(chunks):
            res[b, u * step : (u + 1) * step] = nn(comb[b, 0, u], wo[hme]) + nn(
                comb[b, 1, u], wp[hme]
            )

    def close(b):
        for u in range(chunks):
            for pair in range(pairs - 1):
                ref = part_in.at[b, pair, u]
                remote(ref, ref, p_send.at[b, 0], p_recv.at[b, u, pair], "head", mate).wait_recv()
                here = slice(u * step, (u + 1) * step)
                res[b, here] = res[b, here] + part_in[b, pair, u].astype(F32)

        q_v[b * rows : (b + 1) * rows] = res[b].astype(BF)
        copy = pltpu.make_async_copy(
            q_v.at[pl.ds(b * rows, rows)], mixed_h.at[b], out_sem.at[1 + b]
        )
        copy.start()
        return copy

    for t in range(nh):

        @pl.when(wo_gets(t))
        def _():
            wo_copy(t).wait_recv()
            wo_pass(t).start()

    if fine:
        for c in evens:
            if c & (c - 1):
                from_mate(0, c + 1)
                visit(c)
    else:
        for c in evens:
            from_mate(0, c + 1)
        visit_all(0)
    combine(0)

    def ns_steps(mats, count, norms=None):
        def one(_, carry):
            for at, i in enumerate(mats):
                x = grad[0, i] if norms is None else grad[0, i] * norms[at]
                xb = x.astype(BF)
                gram = nt(xb, xb)
                gb = gram.astype(BF)
                poly = coeff_b * gram + coeff_c * nn(gb, gb)
                grad[0, i] = coeff_a * x + nn(poly.astype(BF), xb)
            return carry

        if count == 1:
            one(0, 0)
        else:
            lax.fori_loop(0, count, one, 0)

    for own in range(2):

        @pl.when(core == own)
        def _():
            norms = []
            for i in owned[own]:
                g_copy(i).wait_recv()
                g = grad[0, i] + g_in[i].astype(F32)
                grad[0, i] = g
                norms.append(lax.rsqrt(jnp.sum(g * g) + norm_eps))
            ns_steps(owned[own], 1, norms)

    first_hops(1)
    for own in range(2):

        @pl.when(core == own)
        def _():
            ns_steps(owned[own], 2)

    for t in range(nh):

        @pl.when(wo_gets(t))
        def _():
            wo_pass(t).wait_recv()

    in_wo.wait()
    cross(0)
    near_hops(1)
    for own in range(2):

        @pl.when(core == own)
        def _():
            ns_steps(owned[own], NS_STEPS - 4)

    far_hops(1)
    for own in range(2):

        @pl.when(core == own)
        def _():
            ns_steps(owned[own], 1)
            for i in owned[own]:
                g_out[i] = grad[0, i].astype(BF)
                x_copy(i).start()

    from_mate(1, 1)
    if fine:
        for far in (False, True):
            chips = [c for c in evens if far == (c & (c - 1) != 0)]
            for c in chips:
                from_mate(1, c + 1)
            visit_before([] if far else [1], chips)
    else:
        for c in evens:
            from_mate(1, c + 1)
        visit_all(1)

    def stepped(own, i):
        moved = g_out[i] if i in owned[own] else g_in[i]
        return f_v[i] - fast_step * moved.astype(F32)

    for own in range(2):

        @pl.when(core == own)
        def _():
            for i in owned[1 - own]:
                x_copy(i).wait_recv()
            for i in range(3):
                fb[i] = stepped(own, i).astype(BF)

    fast_out(1, fb)
    combine(1)
    for own in range(2):

        @pl.when(core == own)
        def _():
            for i in range(3):
                f_v[i] = stepped(own, i)

    outs = (o1_h, o3_h, o2_h)
    writes = [pltpu.make_async_copy(f_v.at[i], outs[i], out_sem.at[0]) for i in range(3)]
    for copy in writes:
        copy.start()
    writes = [pltpu.make_async_copy(f_v, f_v, out_sem.at[0])]
    writes.append(close(0))
    cross(1)
    writes.append(close(1))
    for copy in writes:
        copy.wait()
    kv_sent()
    all_rates.wait_send()
    for b in range(2):
        ref = comb.at[b, 0]
        remote(ref, ref, c_send.at[b], c_recv.at[b, 0], "head", mate).wait_send()
    for own in range(2):

        @pl.when(core == own)
        def _():
            for i in owned[1 - own]:
                g_copy(i).wait_send()
            for i in owned[own]:
                x_copy(i).wait_send()

    for t in range(nh):

        @pl.when((mate == t) | crosses(mate, t))
        def _():
            wo_copy(t).wait_send()

        @pl.when(wo_gets(t))
        def _():
            wo_pass(t).wait_send()

        @pl.when(crosses(hme, t))
        def _():
            for b in range(2):
                ref = tok.at[pl.ds(b * rows, rows), pl.ds(t * cols, cols)]
                remote(ref, ref, p_send.at[b, t], p_recv.at[0, 0, 0], "head", mate).wait_send()


def layer(n, nh, rows, flat, w_qkv, w_rate, f1, f3, f2, gain, wo):
    total, width = flat.shape
    blocks = total // rows
    dh, fh = f1.shape
    cols = wo.shape[1] // nh
    chunks = 4
    step = rows // chunks
    dma = pltpu.SemaphoreType.DMA
    buffers = [
        pltpu.VMEM((total, width), BF),
        pltpu.VMEM((3, width, dh), BF),
        pltpu.VMEM((1, width), BF),
        pltpu.VMEM((1, dh), F32),
        pltpu.VMEM((3, dh, fh), F32),
        pltpu.VMEM((3, dh, fh), BF),
        pltpu.VMEM((nh, dh, cols), BF),
        pltpu.VMEM((nh, dh, cols), BF),
        pltpu.VMEM((total, dh), BF),
        pltpu.VMEM((n, 2, total, dh), BF),
        pltpu.VMEM((n // 2, 8, rows), F32),
        pltpu.VMEM((2 if n <= 8 else 1, 3, dh, fh), F32),
        pltpu.VMEM((3, dh, fh), BF),
        pltpu.VMEM((3, dh, fh), BF),
        pltpu.VMEM((blocks, rows, 1), F32),
        pltpu.VMEM((blocks, rows, LANES), F32),
        pltpu.VMEM((blocks, rows, dh), F32),
        pltpu.VMEM((rows, dh), F32),
        pltpu.VMEM((blocks, 2, chunks, step, dh), BF),
        pltpu.VMEM((blocks, nh // 2 - 1, chunks, step, cols), BF),
        pltpu.VMEM((blocks, rows, cols), F32),
    ]
    need = sum(math.prod(b.shape) * jnp.dtype(b.dtype).itemsize for b in buffers)
    return pl.pallas_call(
        functools.partial(layer_kernel, n, nh, rows),
        in_specs=[HBM] * 8,
        out_specs=[ANY] * 4,
        out_shape=[jax.ShapeDtypeStruct((blocks, rows, cols), BF)]
        + [jax.ShapeDtypeStruct(f.shape, F32) for f in (f1, f3, f2)],
        scratch_shapes=[
            *buffers,
            dma((9,)),
            dma((blocks, 2)),
            dma((len(arrivals(n)),)),
            dma,
            dma,
            dma((3,)),
            dma((3,)),
            dma((2, nh)),
            dma((2, nh)),
            dma((blocks,)),
            dma((blocks, chunks)),
            dma((blocks, nh)),
            dma((blocks, chunks, nh // 2 - 1)),
            dma((1 + blocks,)),
        ],
        compiler_params=pltpu.CompilerParams(
            vmem_limit_bytes=min(67_000_000, need + 6_000_000), collective_id=0, has_side_effects=True
        ),
        name="layer",
    )(
        *(
            pltpu.with_memory_space_constraint(x, pltpu.HBM)
            for x in (flat, w_qkv, w_rate, f1, f3, f2, gain, wo)
        )
    )


def write_kernel(*refs):
    half = len(refs) // 2
    sems = refs[-1]
    copies = [
        pltpu.make_async_copy(refs[i], refs[half + i], sems.at[i]) for i in range(half)
    ]
    for copy in copies:
        copy.start()
    for copy in copies:
        copy.wait()


def write_out(arrays):
    return pl.pallas_call(
        write_kernel,
        in_specs=[ANY] * len(arrays),
        out_specs=[HBM] * len(arrays),
        out_shape=[jax.ShapeDtypeStruct(a.shape, a.dtype) for a in arrays],
        scratch_shapes=[pltpu.SemaphoreType.DMA((len(arrays),))],
        compiler_params=pltpu.CompilerParams(vmem_limit_bytes=4_000_000),
        name="write_out",
    )(*arrays)


def shards(tokens, w_qkv, w_rate, w_out, fw_gain, fast_first, fast_third, fast_second):
    blocks, rows, width = tokens.shape
    dh = w_out.shape[1]
    done = layer(
        lax.axis_size("ctx"),
        lax.axis_size("head"),
        rows,
        tokens.reshape(blocks * rows, width),
        w_qkv.reshape(width, 3 * dh),
        w_rate.reshape(1, width),
        fast_first[0],
        fast_third[0],
        fast_second[0],
        fw_gain,
        w_out[0],
    )
    mixed, *current = write_out(done)
    return (mixed,) + tuple(f[None] for f in current)


def solution(mesh):
    placed = (
        P(None, "ctx", None),
        P(None, "head", None),
        P(None, "head"),
        P("head", None, None),
        P("head", None),
        P("head", None, None),
        P("head", None, None),
        P("head", None, None),
    )
    return jax.shard_map(
        shards,
        mesh=mesh,
        in_specs=placed,
        out_specs=(
            P(None, "ctx", "head"),
            P("head", None, None),
            P("head", None, None),
            P("head", None, None),
        ),
        check_vma=False,
    )
```

```python
import functools
import math

import jax
import jax.numpy as jnp
from jax import lax
from jax.experimental import pallas as pl
from jax.experimental.pallas import tpu as pltpu
from jax.sharding import PartitionSpec as P

WINDOW = 2048
NS_STEPS = 5

coeff_a = 3.4445
coeff_b = -4.775
coeff_c = 2.0315
fast_step = 0.5
norm_eps = 1e-06
LOG2E = 1.4426950408889634
NEG = -1e30
BF = jnp.bfloat16
F32 = jnp.float32
VMEM = pl.BlockSpec(memory_space=pltpu.VMEM)
ANY = pl.BlockSpec(memory_space=pl.ANY)
HBM = pl.BlockSpec(memory_space=pltpu.HBM)
LANES = 128


def mm(left, right, dims):
    return lax.dot_general(left, right, (dims, ((), ())), preferred_element_type=F32)


def nn(left, right):
    return mm(left, right, ((1,), (0,)))


def nt(left, right):
    return mm(left, right, ((1,), (1,)))


def tn(left, right):
    return mm(left, right, ((0,), (0,)))


def cross_bits(n, sub):
    bits = [1 << i for i in range(1, n.bit_length() - 1)]
    return bits if sub == 0 else bits[::-1]


def arrivals(n):
    slots = {}
    for b in range(2):
        for c in range(1, n):
            for sub in range(2):
                for kv in range(2):
                    if c % 2:
                        key = (b, c, None, None)
                    elif c == cross_bits(n, sub)[0]:
                        key = (b, c, sub, kv)
                    else:
                        key = (b, c, sub, None)
                    slots.setdefault(key, len(slots))
    return slots


def remote(src, dst, send, recv, axis, peer):
    return pltpu.make_async_remote_copy(
        src_ref=src,
        dst_ref=dst,
        send_sem=send,
        recv_sem=recv,
        device_id={axis: peer},
        device_id_type=pl.DeviceIdType.MESH,
    )


def layer_kernel(
    n, nh, rows,
    tok_h, w_h, wr_h, f1_h, f3_h, f2_h, gain_h, wo_h,
    mixed_h, o1_h, o3_h, o2_h,
    tok, w, wr, gain, f_v, fb, wo, wp, q_v, every, rates,
    grad, g_out, g_in,
    m_s, l_s, acc, normed, comb, part_in, res,
    load, k_send, k_recv, s_send, s_recv, e_send, e_recv,
    w_send, w_recv, c_send, c_recv, p_send, p_recv, out_sem,
):
    me = lax.axis_index("ctx")
    hme = lax.axis_index("head")
    dh = q_v.shape[1]
    cols = wo.shape[2]
    reach = WINDOW // rows
    scale = dh ** (-0.5) * LOG2E
    core = lax.rem(me, 2)
    fine = n <= 8
    evens = sorted(range(2, n, 2), key=lambda c: (bin(c).count("1"), c))
    hpair = hme // 2
    hodd = lax.rem(hme, 2)
    mate = hme + 1 - 2 * hodd

    def fetch(i, src, dst):
        copy = pltpu.make_async_copy(src, dst, load.at[i])
        copy.start()
        return copy

    first, second = pl.ds(0, rows), pl.ds(rows, rows)
    in_tok0 = fetch(0, tok_h.at[first], tok.at[first])
    in_k = fetch(1, w_h.at[:, pl.ds(dh, dh)], w.at[1])

    barrier = pltpu.get_barrier_semaphore()
    peers = [1] + evens
    for c in peers:
        pl.semaphore_signal(
            barrier, inc=1, device_id={"ctx": me ^ c}, device_id_type=pl.DeviceIdType.MESH
        )
    for r in range(1, nh):
        pl.semaphore_signal(
            barrier,
            inc=1,
            device_id={"head": lax.rem(hme + r, nh)},
            device_id_type=pl.DeviceIdType.MESH,
        )

    half = rows // 2
    slots = arrivals(n)

    def piece(b, c, sub, kv):
        span = pl.ds(b * rows, rows) if sub is None else pl.ds(b * rows + sub * half, half)
        return every.at[me ^ c, slice(None) if kv is None else kv, span]

    def slot(b, c, sub, kv):
        for key in ((b, c, sub, kv), (b, c, sub, None), (b, c, None, None)):
            if key in slots:
                return slots[key]

    def kv_copy(b, c, sub, kv, bit):
        ref = piece(b, c, sub, kv)
        return remote(
            ref, ref, k_send.at[b, sub], k_recv.at[slot(b, c | bit, sub, kv)], "ctx", me ^ bit
        )

    def kv_wait(b, c, sub=None, kv=None):
        ref = piece(b, c, sub, kv)
        at = k_recv.at[slot(b, c, sub, kv)]
        remote(ref, ref, k_send.at[0, 0], at, "ctx", me ^ (c & -c)).wait_recv()

    def pass_on(b, c, sub, kv):
        order = cross_bits(n, sub)
        last = max(i for i, bit in enumerate(order) if c & bit)
        for bit in order[last + 1 :] + [1]:
            kv_copy(b, c, sub, kv, bit).start()

    def send_own(b, kv, turns):
        for turn in turns:
            for sub in range(2):
                kv_copy(b, 0, sub, kv, cross_bits(n, sub)[turn]).start()
        if 0 in turns:
            for sub in range(2):
                kv_copy(b, 0, sub, kv, 1).start()

    def kv_sent():
        for b in range(2):
            for sub in range(2):
                ref = every.at[pl.ds(0, n - 1), :, pl.ds(0, half)]
                remote(
                    ref, ref, k_send.at[b, sub], k_recv.at[0], "ctx", me ^ 1
                ).wait_send()

    later_turns = range(1, len(cross_bits(n, 0)))

    def hops(b, far, first):
        for c in evens:
            for kv in range(2) if first else (None,):
                for sub in range(2):
                    near = c == cross_bits(n, sub)[0]
                    if far == (c & (c - 1) != 0) and (far or first == near):
                        kv_wait(b, c, sub, kv)
                        pass_on(b, c, sub, kv)

    def first_hops(b):
        hops(b, False, True)

    def near_hops(b):
        hops(b, False, False)

    def far_hops(b):
        hops(b, True, False)

    def from_mate(b, c):
        kv_wait(b, c)

    in_tok0.wait()
    in_k.wait()
    in_v = fetch(2, w_h.at[:, pl.ds(2 * dh, dh)], w.at[2])
    in_wr = fetch(7, wr_h, wr)
    in_gain = fetch(8, gain_h, gain)
    every[me, 0, :rows] = nn(tok[:rows], w[1]).astype(BF)
    pl.semaphore_wait(barrier, len(peers) + nh - 1)
    send_own(0, 0, (0,))
    in_v.wait()
    in_tok1 = fetch(3, tok_h.at[second], tok.at[second])
    in_q = fetch(4, w_h.at[:, pl.ds(0, dh)], w.at[0])
    for i, f in enumerate((f1_h, f3_h, f2_h)):
        fetch(5, f, f_v.at[i])
    in_f = pltpu.make_async_copy(f_v, f_v, load.at[5])
    for t in range(nh):
        fetch(6, wo_h.at[:, pl.ds(t * cols, cols)], wo.at[t])
    in_wo = pltpu.make_async_copy(wo, wo, load.at[6])
    every[me, 1, :rows] = nn(tok[:rows], w[2]).astype(BF)
    send_own(0, 1, (0,))
    send_own(0, None, later_turns)

    def rate_copy(c):
        i = c // 2
        return remote(rates.at[0], rates.at[i], s_send, s_recv, "ctx", me ^ c)

    in_wr.wait()
    logit = nt(jnp.broadcast_to(wr[...], (8, wr.shape[1])), tok[:rows])
    rates[0] = jnp.maximum(logit, 0.0) + jnp.log1p(jnp.exp(-jnp.abs(logit)))
    for c in evens:
        rate_copy(c).start()

    others = rates.at[pl.ds(1, n // 2 - 1)]
    all_rates = remote(others, others, s_send, s_recv, "ctx", me ^ 1)

    def crosses(h, t):
        odd = lax.rem(h, 2)
        up = (odd == 1) & (t // 2 > h // 2)
        down = (odd == 0) & (t // 2 < h // 2)
        return up | down

    share = pl.ds(pl.multiple_of(core * (dh // 2), dh // 2), dh // 2)

    def wo_copy(t):
        return remote(
            wo_h.at[share, pl.ds(t * cols, cols)],
            wp.at[t, share],
            w_send.at[0, t],
            w_recv.at[0, t],
            "head",
            mate,
        )

    def wo_pass(t):
        ref = wp.at[t, share]
        return remote(ref, ref, w_send.at[1, t], w_recv.at[1, t], "ctx", me ^ 1)

    def wo_gets(t):
        return (hme == t) | crosses(hme, t)

    for t in range(nh):

        @pl.when((mate == t) | crosses(mate, t))
        def _():
            wo_copy(t).start()

    in_tok1.wait()
    every[me, 0, rows:] = nn(tok[rows:], w[1]).astype(BF)
    every[me, 1, rows:] = nn(tok[rows:], w[2]).astype(BF)
    in_q.wait()
    in_gain.wait()
    q_v[...] = nn(tok[...], w[0]).astype(BF)
    in_f.wait()
    for i in range(3):
        fb[i] = f_v[i].astype(BF)

    def gradients(s, at, slot, add, close_sum=False):
        keys = every[s, 0, :rows]
        vals = every[s, 1, :rows]
        rate = jnp.transpose(rates[at])[:, :1]
        target = (-rate * vals.astype(F32)).astype(BF)
        h1 = nn(keys, fb[0])
        h3 = nn(keys, fb[1])
        sig = jax.nn.sigmoid(h1)
        silu = h1 * sig
        act = (silu * h3).astype(BF)
        dact = nt(target, fb[2])
        d1 = (dact * h3 * (sig * (1.0 + h1 * (1.0 - sig)))).astype(BF)
        d3 = (dact * silu).astype(BF)
        new = (tn(keys, d1), tn(keys, d3), tn(act, target))
        for i in range(3):
            if close_sum:
                grad[0, i] = grad[0, i] + (grad[1, i] + new[i])
            else:
                grad[slot, i] = grad[slot, i] + new[i] if add else new[i]

    def attend(b, sources, side, gap=None, begin=False, hide=None):
        q = q_v[pl.ds(pl.multiple_of(b * rows, rows), rows)]
        span = pl.ds(side * rows, rows)
        scores = [nt(q, every[s, 0, span]) for s in sources]
        if gap is not None:
            off = (
                lax.broadcasted_iota(jnp.int32, (rows, rows), 0)
                - lax.broadcasted_iota(jnp.int32, (rows, rows), 1)
                + gap * rows
            )
            scores = [jnp.where((off >= 0) & (off < WINDOW), sc, NEG) for sc in scores]
        if hide is not None:
            scores = [sc + bias for sc, bias in zip(scores, hide)]
        top = functools.reduce(jnp.maximum, scores)
        new = jnp.max(top, axis=1, keepdims=True)
        if not begin:
            new = jnp.maximum(m_s[b], new)
        probs = [jnp.exp2((sc - new) * scale) for sc in scores]
        lane = sum(p[:, i : i + LANES] for p in probs for i in range(0, rows, LANES))
        pv = sum(nn(p.astype(BF), every[s, 1, span]) for p, s in zip(probs, sources))
        if begin:
            l_s[b] = lane
            acc[b] = pv
        else:
            fade = jnp.exp2((m_s[b] - new) * scale)
            l_s[b] = l_s[b] * fade + lane
            acc[b] = acc[b] * fade + pv
        m_s[b] = new

    def visit(c):
        sources = [me ^ c] if c == 1 else [me ^ c, me ^ c ^ 1]
        attend(jnp.where(me > me ^ c, 0, 1), sources, 0)

    def visit_before(single, chips):
        sources = [me ^ c for c in single] + [me ^ c ^ i for c in chips for i in range(2)]
        attend(1, sources, 1, hide=[jnp.where(me > s, 0.0, NEG) for s in sources])

    def visit_all(side):
        def one(s, carry):
            gap = me - s
            b = jnp.where(gap >= 0, side, 1)
            gap = gap + (b - side) * n

            @pl.when((s != me) & (gap >= 0) & (gap <= reach))
            def _():
                attend(b, [s], side, gap)

            return carry

        lax.fori_loop(0, n, one, 0)

    def fast_out(b, weights):
        q = q_v[b * rows : (b + 1) * rows]
        h1 = nn(q, weights[0])
        h3 = nn(q, weights[1])
        act = (jax.nn.silu(h1) * h3).astype(BF)
        out = nn(act, weights[2])
        inv = lax.rsqrt(jnp.mean(out * out, axis=1, keepdims=True) + norm_eps)
        normed[...] = out * inv * gain[...]

    if fine:
        gradients(me, 0, 0, False)
    fast_out(0, fb)
    attend(0, [me], 0, 0, True)
    first_hops(0)
    for kv in range(2):
        send_own(1, kv, (0,))
    send_own(1, None, later_turns)
    attend(1, [me], 1, 0, True)
    if n <= reach:
        attend(1, [me], 0, n)
    from_mate(0, 1)
    if fine:
        visit(1)
    near_hops(0)
    all_rates.wait_recv()
    if fine:
        for c in evens:
            if c & (c - 1) == 0:
                gradients(me ^ c, c // 2, c // 4, c < 4)
        for c in evens:
            if c & (c - 1) == 0:
                from_mate(0, c + 1)
                visit(c)
    far_hops(0)
    if fine:
        for c in evens:
            if c & (c - 1):
                gradients(me ^ c, c // 2, 1, True, True)
    else:
        grad[0] = jnp.zeros_like(grad[0])

        def summed(j, carry):
            gradients(2 * j + core, (me // 2) ^ j, 0, True)
            return carry

        lax.fori_loop(0, n // 2, summed, 0)

    def g_copy(i):
        return remote(g_out.at[i], g_in.at[i], e_send.at[i], e_recv.at[i], "ctx", me ^ 1)

    def x_copy(i):
        return remote(g_out.at[i], g_in.at[i], e_send.at[i], e_recv.at[i], "ctx", me ^ 1)

    owned = ((0, 1), (2,))

    for own in range(2):

        @pl.when(core == own)
        def _():
            for i in owned[1 - own]:
                g_out[i] = grad[0, i].astype(BF)
                g_copy(i).start()

    chunks = comb.shape[2]
    pairs = nh // 2
    step = rows // chunks

    def c_copy(b, u):
        return remote(
            comb.at[b, 0, u], comb.at[b, 1, u], c_send.at[b], c_recv.at[b, u], "head", mate
        )

    def spot(b, u):
        return pl.ds(b * rows + u * step, step)

    def p_copy(b, u, t):
        return remote(
            tok.at[spot(b, u), pl.ds(t * cols, cols)],
            part_in.at[b, lax.rem(hpair - t // 2 + pairs, pairs) - 1, u],
            p_send.at[b, t],
            p_recv.at[b, u, lax.rem(hpair - t // 2 + pairs, pairs) - 1],
            "head",
            t,
        )

    def combine(b):
        both = acc[b] / jnp.sum(l_s[b], axis=1, keepdims=True) + normed[...]
        for u in range(chunks):
            comb[b, 0, u] = both[u * step : (u + 1) * step].astype(BF)
            c_copy(b, u).start()

    targets = sorted(range(nh), key=lambda t: -abs(2 * t - nh + 1))

    def cross(b):
        if b == 0:
            for u in range(chunks):
                c_copy(b, u).wait_recv()
        for t in targets:

            @pl.when(crosses(hme, t))
            def _():
                if b == 0:
                    mine, pair = (comb[b, k].reshape(rows, dh) for k in range(2))
                    tok[b * rows : (b + 1) * rows, t * cols : (t + 1) * cols] = (
                        nn(mine, wo[t]) + nn(pair, wp[t])
                    ).astype(BF)
                for u in range(chunks):
                    if b > 0:
                        if t == 0 or t == nh - 1:
                            c_copy(b, u).wait_recv()
                        tok[spot(b, u), t * cols : (t + 1) * cols] = (
                            nn(comb[b, 0, u], wo[t]) + nn(comb[b, 1, u], wp[t])
                        ).astype(BF)
                    p_copy(b, u, t).start()

    def own_part(b):
        if b > 0:

            @pl.when(jnp.logical_not(crosses(hme, 0) | crosses(hme, nh - 1)))
            def _():
                for u in range(chunks):
                    c_copy(b, u).wait_recv()

        mine, pair = (comb[b, k].reshape(rows, dh) for k in range(2))
        res[b] = nn(mine, wo[hme]) + nn(pair, wp[hme])

    def close(b):
        for u in range(chunks):
            for pair in range(pairs - 1):
                ref = part_in.at[b, pair, u]
                remote(ref, ref, p_send.at[b, 0], p_recv.at[b, u, pair], "head", mate).wait_recv()
                here = slice(u * step, (u + 1) * step)
                res[b, here] = res[b, here] + part_in[b, pair, u].astype(F32)

        q_v[b * rows : (b + 1) * rows] = res[b].astype(BF)
        copy = pltpu.make_async_copy(
            q_v.at[pl.ds(b * rows, rows)], mixed_h.at[b], out_sem.at[1 + b]
        )
        copy.start()
        return copy

    for t in range(nh):

        @pl.when(wo_gets(t))
        def _():
            wo_copy(t).wait_recv()
            wo_pass(t).start()

    if fine:
        for c in evens:
            if c & (c - 1):
                from_mate(0, c + 1)
                visit(c)
    else:
        for c in evens:
            from_mate(0, c + 1)
        visit_all(0)
    combine(0)

    def ns_steps(mats, count, norms=None):
        def one(_, carry):
            for at, i in enumerate(mats):
                x = grad[0, i] if norms is None else grad[0, i] * norms[at]
                xb = x.astype(BF)
                gram = nt(xb, xb)
                gb = gram.astype(BF)
                poly = coeff_b * gram + coeff_c * nn(gb, gb)
                grad[0, i] = coeff_a * x + nn(poly.astype(BF), xb)
            return carry

        if count == 1:
            one(0, 0)
        else:
            lax.fori_loop(0, count, one, 0)

    for own in range(2):

        @pl.when(core == own)
        def _():
            norms = []
            for i in owned[own]:
                g_copy(i).wait_recv()
                g = grad[0, i] + g_in[i].astype(F32)
                grad[0, i] = g
                norms.append(lax.rsqrt(jnp.sum(g * g) + norm_eps))
            ns_steps(owned[own], 1, norms)

    first_hops(1)
    for own in range(2):

        @pl.when(core == own)
        def _():
            ns_steps(owned[own], 2)

    for t in range(nh):

        @pl.when(wo_gets(t))
        def _():
            wo_pass(t).wait_recv()

    in_wo.wait()
    cross(0)
    for own in range(2):

        @pl.when(core == own)
        def _():
            ns_steps(owned[own], NS_STEPS - 4)

    near_hops(1)
    for own in range(2):

        @pl.when(core == own)
        def _():
            ns_steps(owned[own], 1)
            for i in owned[own]:
                g_out[i] = grad[0, i].astype(BF)
                x_copy(i).start()

    def second(far):
        chips = [c for c in evens if far == (c & (c - 1) != 0)]
        for c in chips:
            from_mate(1, c + 1)
        visit_before([] if far else [1], chips)

    from_mate(1, 1)
    if fine:
        second(False)
    far_hops(1)

    def stepped(own, i):
        moved = g_out[i] if i in owned[own] else g_in[i]
        return f_v[i] - fast_step * moved.astype(F32)

    for own in range(2):

        @pl.when(core == own)
        def _():
            for i in owned[1 - own]:
                x_copy(i).wait_recv()
            for i in range(3):
                fb[i] = stepped(own, i).astype(BF)

    fast_out(1, fb)
    if fine:
        second(True)
    else:
        for c in evens:
            from_mate(1, c + 1)
        visit_all(1)
    combine(1)
    for own in range(2):

        @pl.when(core == own)
        def _():
            for i in range(3):
                f_v[i] = stepped(own, i)

    outs = (o1_h, o3_h, o2_h)
    writes = [pltpu.make_async_copy(f_v.at[i], outs[i], out_sem.at[0]) for i in range(3)]
    for copy in writes:
        copy.start()
    writes = [pltpu.make_async_copy(f_v, f_v, out_sem.at[0])]
    own_part(0)
    cross(1)
    own_part(1)
    writes.append(close(0))
    writes.append(close(1))
    for copy in writes:
        copy.wait()
    kv_sent()
    all_rates.wait_send()
    for b in range(2):
        ref = comb.at[b, 0]
        remote(ref, ref, c_send.at[b], c_recv.at[b, 0], "head", mate).wait_send()
    for own in range(2):

        @pl.when(core == own)
        def _():
            for i in owned[1 - own]:
                g_copy(i).wait_send()
            for i in owned[own]:
                x_copy(i).wait_send()

    for t in range(nh):

        @pl.when((mate == t) | crosses(mate, t))
        def _():
            wo_copy(t).wait_send()

        @pl.when(wo_gets(t))
        def _():
            wo_pass(t).wait_send()

        @pl.when(crosses(hme, t))
        def _():
            for b in range(2):
                ref = tok.at[pl.ds(b * rows, rows), pl.ds(t * cols, cols)]
                remote(ref, ref, p_send.at[b, t], p_recv.at[0, 0, 0], "head", mate).wait_send()


def layer(n, nh, rows, flat, w_qkv, w_rate, f1, f3, f2, gain, wo):
    total, width = flat.shape
    blocks = total // rows
    dh, fh = f1.shape
    cols = wo.shape[1] // nh
    chunks = 4
    step = rows // chunks
    dma = pltpu.SemaphoreType.DMA
    buffers = [
        pltpu.VMEM((total, width), BF),
        pltpu.VMEM((3, width, dh), BF),
        pltpu.VMEM((1, width), BF),
        pltpu.VMEM((1, dh), F32),
        pltpu.VMEM((3, dh, fh), F32),
        pltpu.VMEM((3, dh, fh), BF),
        pltpu.VMEM((nh, dh, cols), BF),
        pltpu.VMEM((nh, dh, cols), BF),
        pltpu.VMEM((total, dh), BF),
        pltpu.VMEM((n, 2, total, dh), BF),
        pltpu.VMEM((n // 2, 8, rows), F32),
        pltpu.VMEM((2 if n <= 8 else 1, 3, dh, fh), F32),
        pltpu.VMEM((3, dh, fh), BF),
        pltpu.VMEM((3, dh, fh), BF),
        pltpu.VMEM((blocks, rows, 1), F32),
        pltpu.VMEM((blocks, rows, LANES), F32),
        pltpu.VMEM((blocks, rows, dh), F32),
        pltpu.VMEM((rows, dh), F32),
        pltpu.VMEM((blocks, 2, chunks, step, dh), BF),
        pltpu.VMEM((blocks, nh // 2 - 1, chunks, step, cols), BF),
        pltpu.VMEM((blocks, rows, cols), F32),
    ]
    need = sum(math.prod(b.shape) * jnp.dtype(b.dtype).itemsize for b in buffers)
    return pl.pallas_call(
        functools.partial(layer_kernel, n, nh, rows),
        in_specs=[HBM] * 8,
        out_specs=[ANY] * 4,
        out_shape=[jax.ShapeDtypeStruct((blocks, rows, cols), BF)]
        + [jax.ShapeDtypeStruct(f.shape, F32) for f in (f1, f3, f2)],
        scratch_shapes=[
            *buffers,
            dma((9,)),
            dma((blocks, 2)),
            dma((len(arrivals(n)),)),
            dma,
            dma,
            dma((3,)),
            dma((3,)),
            dma((2, nh)),
            dma((2, nh)),
            dma((blocks,)),
            dma((blocks, chunks)),
            dma((blocks, nh)),
            dma((blocks, chunks, nh // 2 - 1)),
            dma((1 + blocks,)),
        ],
        compiler_params=pltpu.CompilerParams(
            vmem_limit_bytes=min(67_000_000, need + 6_000_000), collective_id=0, has_side_effects=True
        ),
        name="layer",
    )(
        *(
            pltpu.with_memory_space_constraint(x, pltpu.HBM)
            for x in (flat, w_qkv, w_rate, f1, f3, f2, gain, wo)
        )
    )


def write_kernel(*refs):
    half = len(refs) // 2
    sems = refs[-1]
    copies = [
        pltpu.make_async_copy(refs[i], refs[half + i], sems.at[i]) for i in range(half)
    ]
    for copy in copies:
        copy.start()
    for copy in copies:
        copy.wait()


def write_out(arrays):
    return pl.pallas_call(
        write_kernel,
        in_specs=[ANY] * len(arrays),
        out_specs=[HBM] * len(arrays),
        out_shape=[jax.ShapeDtypeStruct(a.shape, a.dtype) for a in arrays],
        scratch_shapes=[pltpu.SemaphoreType.DMA((len(arrays),))],
        compiler_params=pltpu.CompilerParams(vmem_limit_bytes=4_000_000),
        name="write_out",
    )(*arrays)


def shards(tokens, w_qkv, w_rate, w_out, fw_gain, fast_first, fast_third, fast_second):
    blocks, rows, width = tokens.shape
    dh = w_out.shape[1]
    done = layer(
        lax.axis_size("ctx"),
        lax.axis_size("head"),
        rows,
        tokens.reshape(blocks * rows, width),
        w_qkv.reshape(width, 3 * dh),
        w_rate.reshape(1, width),
        fast_first[0],
        fast_third[0],
        fast_second[0],
        fw_gain,
        w_out[0],
    )
    mixed, *current = write_out(done)
    return (mixed,) + tuple(f[None] for f in current)


def solution(mesh):
    placed = (
        P(None, "ctx", None),
        P(None, "head", None),
        P(None, "head"),
        P("head", None, None),
        P("head", None),
        P("head", None, None),
        P("head", None, None),
        P("head", None, None),
    )
    return jax.shard_map(
        shards,
        mesh=mesh,
        in_specs=placed,
        out_specs=(
            P(None, "ctx", "head"),
            P("head", None, None),
            P("head", None, None),
            P("head", None, None),
        ),
        check_vma=False,
    )
```

```python
import functools
import math

import jax
import jax.numpy as jnp
from jax import lax
from jax.experimental import pallas as pl
from jax.experimental.pallas import tpu as pltpu
from jax.sharding import PartitionSpec as P

WINDOW = 2048
NS_STEPS = 5

coeff_a = 3.4445
coeff_b = -4.775
coeff_c = 2.0315
fast_step = 0.5
norm_eps = 1e-06
LOG2E = 1.4426950408889634
NEG = -1e30
BF = jnp.bfloat16
F32 = jnp.float32
VMEM = pl.BlockSpec(memory_space=pltpu.VMEM)
ANY = pl.BlockSpec(memory_space=pl.ANY)
HBM = pl.BlockSpec(memory_space=pltpu.HBM)
LANES = 128


def mm(left, right, dims):
    return lax.dot_general(left, right, (dims, ((), ())), preferred_element_type=F32)


def nn(left, right):
    return mm(left, right, ((1,), (0,)))


def nt(left, right):
    return mm(left, right, ((1,), (1,)))


def tn(left, right):
    return mm(left, right, ((0,), (0,)))


def cross_bits(n, sub):
    bits = [1 << i for i in range(1, n.bit_length() - 1)]
    return bits if sub == 0 else bits[::-1]


def arrivals(n):
    slots = {}
    for b in range(2):
        for c in range(1, n):
            for sub in range(2):
                for kv in range(2):
                    if c % 2:
                        key = (b, c, None, None)
                    elif c == cross_bits(n, sub)[0]:
                        key = (b, c, sub, kv)
                    else:
                        key = (b, c, sub, None)
                    slots.setdefault(key, len(slots))
    return slots


def remote(src, dst, send, recv, axis, peer):
    return pltpu.make_async_remote_copy(
        src_ref=src,
        dst_ref=dst,
        send_sem=send,
        recv_sem=recv,
        device_id={axis: peer},
        device_id_type=pl.DeviceIdType.MESH,
    )


def layer_kernel(
    n, nh, rows,
    tok_h, w_h, wr_h, f1_h, f3_h, f2_h, gain_h, wo_h,
    mixed_h, o1_h, o3_h, o2_h,
    tok, w, wr, gain, f_v, fb, wo, wp, q_v, every, rates,
    grad, g_out, g_in,
    m_s, l_s, acc, normed, comb, part_in, res,
    load, k_send, k_recv, s_send, s_recv, e_send, e_recv,
    w_send, w_recv, c_send, c_recv, p_send, p_recv, out_sem,
):
    me = lax.axis_index("ctx")
    hme = lax.axis_index("head")
    dh = q_v.shape[1]
    cols = wo.shape[2]
    reach = WINDOW // rows
    scale = dh ** (-0.5) * LOG2E
    core = lax.rem(me, 2)
    fine = n <= 8
    evens = sorted(range(2, n, 2), key=lambda c: (bin(c).count("1"), c))
    hpair = hme // 2
    hodd = lax.rem(hme, 2)
    mate = hme + 1 - 2 * hodd

    def fetch(i, src, dst):
        copy = pltpu.make_async_copy(src, dst, load.at[i])
        copy.start()
        return copy

    first, second = pl.ds(0, rows), pl.ds(rows, rows)
    def fetch_rows(i, src, dst, parts):
        size = dst.shape[0] // parts
        for at in range(0, dst.shape[0], size):
            fetch(i, src.at[pl.ds(at, size)], dst.at[pl.ds(at, size)])
        return pltpu.make_async_copy(dst, dst, load.at[i])

    in_tok0 = fetch_rows(0, tok_h.at[first], tok.at[first], 2)
    in_k = fetch_rows(1, w_h.at[:, pl.ds(dh, dh)], w.at[1], 4)

    barrier = pltpu.get_barrier_semaphore()
    peers = [1] + evens
    for c in peers:
        pl.semaphore_signal(
            barrier, inc=1, device_id={"ctx": me ^ c}, device_id_type=pl.DeviceIdType.MESH
        )
    for r in range(1, nh):
        pl.semaphore_signal(
            barrier,
            inc=1,
            device_id={"head": lax.rem(hme + r, nh)},
            device_id_type=pl.DeviceIdType.MESH,
        )

    half = rows // 2
    slots = arrivals(n)

    def piece(b, c, sub, kv):
        span = pl.ds(b * rows, rows) if sub is None else pl.ds(b * rows + sub * half, half)
        return every.at[me ^ c, slice(None) if kv is None else kv, span]

    def slot(b, c, sub, kv):
        for key in ((b, c, sub, kv), (b, c, sub, None), (b, c, None, None)):
            if key in slots:
                return slots[key]

    def kv_copy(b, c, sub, kv, bit):
        ref = piece(b, c, sub, kv)
        return remote(
            ref, ref, k_send.at[b, sub], k_recv.at[slot(b, c | bit, sub, kv)], "ctx", me ^ bit
        )

    def kv_wait(b, c, sub=None, kv=None):
        ref = piece(b, c, sub, kv)
        at = k_recv.at[slot(b, c, sub, kv)]
        remote(ref, ref, k_send.at[0, 0], at, "ctx", me ^ (c & -c)).wait_recv()

    def pass_on(b, c, sub, kv):
        order = cross_bits(n, sub)
        last = max(i for i, bit in enumerate(order) if c & bit)
        for bit in order[last + 1 :] + [1]:
            kv_copy(b, c, sub, kv, bit).start()

    def send_own(b, kv, turns):
        for turn in turns:
            for sub in range(2):
                kv_copy(b, 0, sub, kv, cross_bits(n, sub)[turn]).start()
        if 0 in turns:
            for sub in range(2):
                kv_copy(b, 0, sub, kv, 1).start()

    def kv_sent():
        for b in range(2):
            for sub in range(2):
                ref = every.at[pl.ds(0, n - 1), :, pl.ds(0, half)]
                remote(
                    ref, ref, k_send.at[b, sub], k_recv.at[0], "ctx", me ^ 1
                ).wait_send()

    later_turns = range(1, len(cross_bits(n, 0)))

    def hops(b, far, first):
        for c in evens:
            for kv in range(2) if first else (None,):
                for sub in range(2):
                    near = c == cross_bits(n, sub)[0]
                    if far == (c & (c - 1) != 0) and (far or first == near):
                        kv_wait(b, c, sub, kv)
                        pass_on(b, c, sub, kv)

    def first_hops(b):
        hops(b, False, True)

    def near_hops(b):
        hops(b, False, False)

    def far_hops(b):
        hops(b, True, False)

    def from_mate(b, c):
        kv_wait(b, c)

    in_tok0.wait()
    in_k.wait()
    in_v = fetch_rows(2, w_h.at[:, pl.ds(2 * dh, dh)], w.at[2], 4)
    in_wr = fetch(7, wr_h, wr)
    in_gain = fetch(8, gain_h, gain)
    every[me, 0, :rows] = nn(tok[:rows], w[1]).astype(BF)
    pl.semaphore_wait(barrier, len(peers) + nh - 1)
    send_own(0, 0, (0,))
    in_v.wait()
    in_tok1 = fetch(3, tok_h.at[second], tok.at[second])
    in_q = fetch(4, w_h.at[:, pl.ds(0, dh)], w.at[0])
    for i, f in enumerate((f1_h, f3_h, f2_h)):
        fetch(5, f, f_v.at[i])
    in_f = pltpu.make_async_copy(f_v, f_v, load.at[5])
    for t in range(nh):
        fetch(6, wo_h.at[:, pl.ds(t * cols, cols)], wo.at[t])
    in_wo = pltpu.make_async_copy(wo, wo, load.at[6])
    every[me, 1, :rows] = nn(tok[:rows], w[2]).astype(BF)
    send_own(0, 1, (0,))
    send_own(0, None, later_turns)

    def rate_copy(c):
        i = c // 2
        return remote(rates.at[0], rates.at[i], s_send, s_recv, "ctx", me ^ c)

    in_wr.wait()
    logit = nt(jnp.broadcast_to(wr[...], (8, wr.shape[1])), tok[:rows])
    rates[0] = jnp.maximum(logit, 0.0) + jnp.log1p(jnp.exp(-jnp.abs(logit)))
    for c in evens:
        rate_copy(c).start()

    others = rates.at[pl.ds(1, n // 2 - 1)]
    all_rates = remote(others, others, s_send, s_recv, "ctx", me ^ 1)

    def crosses(h, t):
        odd = lax.rem(h, 2)
        up = (odd == 1) & (t // 2 > h // 2)
        down = (odd == 0) & (t // 2 < h // 2)
        return up | down

    share = pl.ds(pl.multiple_of(core * (dh // 2), dh // 2), dh // 2)

    def wo_copy(t):
        return remote(
            wo_h.at[share, pl.ds(t * cols, cols)],
            wp.at[t, share],
            w_send.at[0, t],
            w_recv.at[0, t],
            "head",
            mate,
        )

    def wo_pass(t):
        ref = wp.at[t, share]
        return remote(ref, ref, w_send.at[1, t], w_recv.at[1, t], "ctx", me ^ 1)

    def wo_gets(t):
        return (hme == t) | crosses(hme, t)

    for t in range(nh):

        @pl.when((mate == t) | crosses(mate, t))
        def _():
            wo_copy(t).start()

    in_tok1.wait()
    every[me, 0, rows:] = nn(tok[rows:], w[1]).astype(BF)
    every[me, 1, rows:] = nn(tok[rows:], w[2]).astype(BF)
    in_q.wait()
    in_gain.wait()
    q_v[...] = nn(tok[...], w[0]).astype(BF)
    in_f.wait()
    for i in range(3):
        fb[i] = f_v[i].astype(BF)

    def gradients(s, at, slot, add, close_sum=False):
        keys = every[s, 0, :rows]
        vals = every[s, 1, :rows]
        rate = jnp.transpose(rates[at])[:, :1]
        target = (-rate * vals.astype(F32)).astype(BF)
        h1 = nn(keys, fb[0])
        h3 = nn(keys, fb[1])
        sig = jax.nn.sigmoid(h1)
        silu = h1 * sig
        act = (silu * h3).astype(BF)
        dact = nt(target, fb[2])
        d1 = (dact * h3 * (sig * (1.0 + h1 * (1.0 - sig)))).astype(BF)
        d3 = (dact * silu).astype(BF)
        new = (tn(keys, d1), tn(keys, d3), tn(act, target))
        for i in range(3):
            if close_sum:
                grad[0, i] = grad[0, i] + (grad[1, i] + new[i])
            else:
                grad[slot, i] = grad[slot, i] + new[i] if add else new[i]

    def attend(b, sources, side, gap=None, begin=False, hide=None):
        q = q_v[pl.ds(pl.multiple_of(b * rows, rows), rows)]
        span = pl.ds(side * rows, rows)
        scores = [nt(q, every[s, 0, span]) for s in sources]
        if gap is not None:
            off = (
                lax.broadcasted_iota(jnp.int32, (rows, rows), 0)
                - lax.broadcasted_iota(jnp.int32, (rows, rows), 1)
                + gap * rows
            )
            scores = [jnp.where((off >= 0) & (off < WINDOW), sc, NEG) for sc in scores]
        if hide is not None:
            scores = [sc + bias for sc, bias in zip(scores, hide)]
        top = functools.reduce(jnp.maximum, scores)
        new = jnp.max(top, axis=1, keepdims=True)
        if not begin:
            new = jnp.maximum(m_s[b], new)
        probs = [jnp.exp2((sc - new) * scale) for sc in scores]
        lane = sum(p[:, i : i + LANES] for p in probs for i in range(0, rows, LANES))
        pv = sum(nn(p.astype(BF), every[s, 1, span]) for p, s in zip(probs, sources))
        if begin:
            l_s[b] = lane
            acc[b] = pv
        else:
            fade = jnp.exp2((m_s[b] - new) * scale)
            l_s[b] = l_s[b] * fade + lane
            acc[b] = acc[b] * fade + pv
        m_s[b] = new

    def visit(c):
        sources = [me ^ c] if c == 1 else [me ^ c, me ^ c ^ 1]
        attend(jnp.where(me > me ^ c, 0, 1), sources, 0)

    def visit_before(single, chips):
        sources = [me ^ c for c in single] + [me ^ c ^ i for c in chips for i in range(2)]
        attend(1, sources, 1, hide=[jnp.where(me > s, 0.0, NEG) for s in sources])

    def visit_all(side):
        def one(s, carry):
            gap = me - s
            b = jnp.where(gap >= 0, side, 1)
            gap = gap + (b - side) * n

            @pl.when((s != me) & (gap >= 0) & (gap <= reach))
            def _():
                attend(b, [s], side, gap)

            return carry

        lax.fori_loop(0, n, one, 0)

    def fast_out(b, weights):
        q = q_v[b * rows : (b + 1) * rows]
        h1 = nn(q, weights[0])
        h3 = nn(q, weights[1])
        act = (jax.nn.silu(h1) * h3).astype(BF)
        out = nn(act, weights[2])
        inv = lax.rsqrt(jnp.mean(out * out, axis=1, keepdims=True) + norm_eps)
        normed[...] = out * inv * gain[...]

    if fine:
        gradients(me, 0, 0, False)
    fast_out(0, fb)
    attend(0, [me], 0, 0, True)
    first_hops(0)
    for kv in range(2):
        send_own(1, kv, (0,))
    send_own(1, None, later_turns)
    attend(1, [me], 1, 0, True)
    if n <= reach:
        attend(1, [me], 0, n)
    from_mate(0, 1)
    if fine:
        visit(1)
    near_hops(0)
    all_rates.wait_recv()
    if fine:
        for c in evens:
            if c & (c - 1) == 0:
                gradients(me ^ c, c // 2, c // 4, c < 4)
        for c in evens:
            if c & (c - 1) == 0:
                from_mate(0, c + 1)
                visit(c)
    far_hops(0)
    if fine:
        for c in evens:
            if c & (c - 1):
                gradients(me ^ c, c // 2, 1, True, True)
    else:
        grad[0] = jnp.zeros_like(grad[0])

        def summed(j, carry):
            gradients(2 * j + core, (me // 2) ^ j, 0, True)
            return carry

        lax.fori_loop(0, n // 2, summed, 0)

    def g_copy(i):
        return remote(g_out.at[i], g_in.at[i], e_send.at[i], e_recv.at[i], "ctx", me ^ 1)

    def x_copy(i):
        return remote(g_out.at[i], g_in.at[i], e_send.at[i], e_recv.at[i], "ctx", me ^ 1)

    owned = ((0, 1), (2,))

    for own in range(2):

        @pl.when(core == own)
        def _():
            for i in owned[1 - own]:
                g_out[i] = grad[0, i].astype(BF)
                g_copy(i).start()

    chunks = comb.shape[2]
    pairs = nh // 2
    step = rows // chunks

    def c_copy(b, u):
        return remote(
            comb.at[b, 0, u], comb.at[b, 1, u], c_send.at[b], c_recv.at[b, u], "head", mate
        )

    def spot(b, u):
        return pl.ds(b * rows + u * step, step)

    def p_copy(b, u, t):
        return remote(
            tok.at[spot(b, u), pl.ds(t * cols, cols)],
            part_in.at[b, lax.rem(hpair - t // 2 + pairs, pairs) - 1, u],
            p_send.at[b, t],
            p_recv.at[b, u, lax.rem(hpair - t // 2 + pairs, pairs) - 1],
            "head",
            t,
        )

    def combine(b):
        both = acc[b] / jnp.sum(l_s[b], axis=1, keepdims=True) + normed[...]
        for u in range(chunks):
            comb[b, 0, u] = both[u * step : (u + 1) * step].astype(BF)
            c_copy(b, u).start()

    targets = sorted(range(nh), key=lambda t: -abs(2 * t - nh + 1))

    def cross(b):
        if b == 0:
            for u in range(chunks):
                c_copy(b, u).wait_recv()
        for t in targets:

            @pl.when(crosses(hme, t))
            def _():
                if b == 0:
                    mine, pair = (comb[b, k].reshape(rows, dh) for k in range(2))
                    tok[b * rows : (b + 1) * rows, t * cols : (t + 1) * cols] = (
                        nn(mine, wo[t]) + nn(pair, wp[t])
                    ).astype(BF)
                for u in range(chunks):
                    if b > 0:
                        if t == 0 or t == nh - 1:
                            c_copy(b, u).wait_recv()
                        tok[spot(b, u), t * cols : (t + 1) * cols] = (
                            nn(comb[b, 0, u], wo[t]) + nn(comb[b, 1, u], wp[t])
                        ).astype(BF)
                    p_copy(b, u, t).start()

    def own_part(b):
        if b > 0:

            @pl.when(jnp.logical_not(crosses(hme, 0) | crosses(hme, nh - 1)))
            def _():
                for u in range(chunks):
                    c_copy(b, u).wait_recv()

        mine, pair = (comb[b, k].reshape(rows, dh) for k in range(2))
        res[b] = nn(mine, wo[hme]) + nn(pair, wp[hme])

    def close(b):
        for u in range(chunks):
            for pair in range(pairs - 1):
                ref = part_in.at[b, pair, u]
                remote(ref, ref, p_send.at[b, 0], p_recv.at[b, u, pair], "head", mate).wait_recv()
                here = slice(u * step, (u + 1) * step)
                res[b, here] = res[b, here] + part_in[b, pair, u].astype(F32)

        q_v[b * rows : (b + 1) * rows] = res[b].astype(BF)
        copy = pltpu.make_async_copy(
            q_v.at[pl.ds(b * rows, rows)], mixed_h.at[b], out_sem.at[1 + b]
        )
        copy.start()
        return copy

    for t in range(nh):

        @pl.when(wo_gets(t))
        def _():
            wo_copy(t).wait_recv()
            wo_pass(t).start()

    if fine:
        for c in evens:
            if c & (c - 1):
                from_mate(0, c + 1)
                visit(c)
    else:
        for c in evens:
            from_mate(0, c + 1)
        visit_all(0)
    combine(0)

    def ns_step(i, norm=None):
        x = grad[0, i]
        xb = x.astype(BF)
        gram = nt(xb, xb)
        if norm is not None:
            gram = gram * (norm * norm)
        gb = gram.astype(BF)
        poly = coeff_b * gram + coeff_c * nn(gb, gb)
        new = coeff_a * x + nn(poly.astype(BF), xb)
        grad[0, i] = new if norm is None else new * norm

    def ns_steps(mats, count):
        def one(_, carry):
            for i in mats:
                ns_step(i)
            return carry

        lax.fori_loop(0, count, one, 0)

    for own in range(2):

        @pl.when(core == own)
        def _():
            for i in owned[own]:
                g_copy(i).wait_recv()
            norms = []
            for i in owned[own]:
                g = grad[0, i] + g_in[i].astype(F32)
                grad[0, i] = g
                norms.append(lax.rsqrt(jnp.sum(g * g) + norm_eps))
            for i, norm in zip(owned[own], norms):
                ns_step(i, norm)

    for count in range(2):
        if count == 1:
            first_hops(1)
        for own in range(2):

            @pl.when(core == own)
            def _():
                ns_steps(owned[own], 1)

    for own in range(2):

        @pl.when(core == own)
        def _():
            ns_steps(owned[own], NS_STEPS - 4)

    near_hops(1)
    for t in range(nh):

        @pl.when(wo_gets(t))
        def _():
            wo_pass(t).wait_recv()

    in_wo.wait()
    cross(0)
    for own in range(2):

        @pl.when(core == own)
        def _():
            for i in owned[own]:
                ns_step(i)
                g_out[i] = grad[0, i].astype(BF)
                x_copy(i).start()

    def second(far):
        chips = [c for c in evens if far == (c & (c - 1) != 0)]
        for c in chips:
            from_mate(1, c + 1)
        visit_before([] if far else [1], chips)

    from_mate(1, 1)

    if fine:
        second(False)
    far_hops(1)

    def stepped(own, i):
        moved = g_out[i] if i in owned[own] else g_in[i]
        return f_v[i] - fast_step * moved.astype(F32)

    for own in range(2):

        @pl.when(core == own)
        def _():
            for i in owned[1 - own]:
                x_copy(i).wait_recv()
            for i in range(3):
                fb[i] = stepped(own, i).astype(BF)

    if fine:
        fast_out(1, fb)
        second(True)
        combine(1)
    else:
        fast_out(1, fb)
        for c in evens:
            from_mate(1, c + 1)
        visit_all(1)
        combine(1)
    for own in range(2):

        @pl.when(core == own)
        def _():
            for i in range(3):
                f_v[i] = stepped(own, i)

    outs = (o1_h, o3_h, o2_h)
    writes = [pltpu.make_async_copy(f_v.at[i], outs[i], out_sem.at[0]) for i in range(3)]
    for copy in writes:
        copy.start()
    writes = [pltpu.make_async_copy(f_v, f_v, out_sem.at[0])]
    own_part(0)
    cross(1)
    own_part(1)
    writes.append(close(0))
    writes.append(close(1))
    for copy in writes:
        copy.wait()
    kv_sent()
    all_rates.wait_send()
    for b in range(2):
        ref = comb.at[b, 0]
        remote(ref, ref, c_send.at[b], c_recv.at[b, 0], "head", mate).wait_send()
    for own in range(2):

        @pl.when(core == own)
        def _():
            for i in owned[1 - own]:
                g_copy(i).wait_send()
            for i in owned[own]:
                x_copy(i).wait_send()

    for t in range(nh):

        @pl.when((mate == t) | crosses(mate, t))
        def _():
            wo_copy(t).wait_send()

        @pl.when(wo_gets(t))
        def _():
            wo_pass(t).wait_send()

        @pl.when(crosses(hme, t))
        def _():
            for b in range(2):
                ref = tok.at[pl.ds(b * rows, rows), pl.ds(t * cols, cols)]
                remote(ref, ref, p_send.at[b, t], p_recv.at[0, 0, 0], "head", mate).wait_send()


def layer(n, nh, rows, flat, w_qkv, w_rate, f1, f3, f2, gain, wo):
    total, width = flat.shape
    blocks = total // rows
    dh, fh = f1.shape
    cols = wo.shape[1] // nh
    chunks = 4
    step = rows // chunks
    dma = pltpu.SemaphoreType.DMA
    buffers = [
        pltpu.VMEM((total, width), BF),
        pltpu.VMEM((3, width, dh), BF),
        pltpu.VMEM((1, width), BF),
        pltpu.VMEM((1, dh), F32),
        pltpu.VMEM((3, dh, fh), F32),
        pltpu.VMEM((3, dh, fh), BF),
        pltpu.VMEM((nh, dh, cols), BF),
        pltpu.VMEM((nh, dh, cols), BF),
        pltpu.VMEM((total, dh), BF),
        pltpu.VMEM((n, 2, total, dh), BF),
        pltpu.VMEM((n // 2, 8, rows), F32),
        pltpu.VMEM((2 if n <= 8 else 1, 3, dh, fh), F32),
        pltpu.VMEM((3, dh, fh), BF),
        pltpu.VMEM((3, dh, fh), BF),
        pltpu.VMEM((blocks, rows, 1), F32),
        pltpu.VMEM((blocks, rows, LANES), F32),
        pltpu.VMEM((blocks, rows, dh), F32),
        pltpu.VMEM((rows, dh), F32),
        pltpu.VMEM((blocks, 2, chunks, step, dh), BF),
        pltpu.VMEM((blocks, nh // 2 - 1, chunks, step, cols), BF),
        pltpu.VMEM((blocks, rows, cols), F32),
    ]
    need = sum(math.prod(b.shape) * jnp.dtype(b.dtype).itemsize for b in buffers)
    return pl.pallas_call(
        functools.partial(layer_kernel, n, nh, rows),
        in_specs=[HBM] * 8,
        out_specs=[ANY] * 4,
        out_shape=[jax.ShapeDtypeStruct((blocks, rows, cols), BF)]
        + [jax.ShapeDtypeStruct(f.shape, F32) for f in (f1, f3, f2)],
        scratch_shapes=[
            *buffers,
            dma((9,)),
            dma((blocks, 2)),
            dma((len(arrivals(n)),)),
            dma,
            dma,
            dma((3,)),
            dma((3,)),
            dma((2, nh)),
            dma((2, nh)),
            dma((blocks,)),
            dma((blocks, chunks)),
            dma((blocks, nh)),
            dma((blocks, chunks, nh // 2 - 1)),
            dma((1 + blocks,)),
        ],
        compiler_params=pltpu.CompilerParams(
            vmem_limit_bytes=min(67_000_000, need + 6_000_000), collective_id=0, has_side_effects=True
        ),
        name="layer",
    )(
        *(
            pltpu.with_memory_space_constraint(x, pltpu.HBM)
            for x in (flat, w_qkv, w_rate, f1, f3, f2, gain, wo)
        )
    )


def write_kernel(*refs):
    half = len(refs) // 2
    sems = refs[-1]
    copies = [
        pltpu.make_async_copy(refs[i], refs[half + i], sems.at[i]) for i in range(half)
    ]
    for copy in copies:
        copy.start()
    for copy in copies:
        copy.wait()


def write_out(arrays):
    return pl.pallas_call(
        write_kernel,
        in_specs=[ANY] * len(arrays),
        out_specs=[HBM] * len(arrays),
        out_shape=[jax.ShapeDtypeStruct(a.shape, a.dtype) for a in arrays],
        scratch_shapes=[pltpu.SemaphoreType.DMA((len(arrays),))],
        compiler_params=pltpu.CompilerParams(vmem_limit_bytes=4_000_000),
        name="write_out",
    )(*arrays)


def shards(tokens, w_qkv, w_rate, w_out, fw_gain, fast_first, fast_third, fast_second):
    blocks, rows, width = tokens.shape
    dh = w_out.shape[1]
    done = layer(
        lax.axis_size("ctx"),
        lax.axis_size("head"),
        rows,
        tokens.reshape(blocks * rows, width),
        w_qkv.reshape(width, 3 * dh),
        w_rate.reshape(1, width),
        fast_first[0],
        fast_third[0],
        fast_second[0],
        fw_gain,
        w_out[0],
    )
    mixed, *current = write_out(done)
    return (mixed,) + tuple(f[None] for f in current)


def solution(mesh):
    placed = (
        P(None, "ctx", None),
        P(None, "head", None),
        P(None, "head"),
        P("head", None, None),
        P("head", None),
        P("head", None, None),
        P("head", None, None),
        P("head", None, None),
    )
    return jax.shard_map(
        shards,
        mesh=mesh,
        in_specs=placed,
        out_specs=(
            P(None, "ctx", "head"),
            P("head", None, None),
            P("head", None, None),
            P("head", None, None),
        ),
        check_vma=False,
    )
```

```python
import functools
import math

import jax
import jax.numpy as jnp
from jax import lax
from jax.experimental import pallas as pl
from jax.experimental.pallas import tpu as pltpu
from jax.sharding import PartitionSpec as P

WINDOW = 2048
NS_STEPS = 5

coeff_a = 3.4445
coeff_b = -4.775
coeff_c = 2.0315
fast_step = 0.5
norm_eps = 1e-06
LOG2E = 1.4426950408889634
NEG = -1e30
BF = jnp.bfloat16
F32 = jnp.float32
VMEM = pl.BlockSpec(memory_space=pltpu.VMEM)
ANY = pl.BlockSpec(memory_space=pl.ANY)
HBM = pl.BlockSpec(memory_space=pltpu.HBM)
LANES = 128


def mm(left, right, dims):
    return lax.dot_general(left, right, (dims, ((), ())), preferred_element_type=F32)


def nn(left, right):
    return mm(left, right, ((1,), (0,)))


def nt(left, right):
    return mm(left, right, ((1,), (1,)))


def tn(left, right):
    return mm(left, right, ((0,), (0,)))


def cross_bits(n, sub):
    bits = [1 << i for i in range(1, n.bit_length() - 1)]
    return bits if sub == 0 else bits[::-1]


def arrivals(n):
    slots = {}
    for b in range(2):
        for c in range(1, n):
            for sub in range(2):
                for kv in range(2):
                    if c % 2:
                        key = (b, c, None, None)
                    elif c == cross_bits(n, sub)[0]:
                        key = (b, c, sub, kv)
                    else:
                        key = (b, c, sub, None)
                    slots.setdefault(key, len(slots))
    return slots


def remote(src, dst, send, recv, axis, peer):
    return pltpu.make_async_remote_copy(
        src_ref=src,
        dst_ref=dst,
        send_sem=send,
        recv_sem=recv,
        device_id={axis: peer},
        device_id_type=pl.DeviceIdType.MESH,
    )


def layer_kernel(
    n, nh, rows,
    tok_h, w_h, wr_h, f1_h, f3_h, f2_h, gain_h, wo_h,
    mixed_h, o1_h, o3_h, o2_h,
    tok, w, wr, gain, f_v, fb, wo, wp, q_v, every, rates,
    grad, g_out, g_in,
    m_s, l_s, acc, normed, comb, part_in, res,
    load, k_send, k_recv, s_send, s_recv, e_send, e_recv,
    w_send, w_recv, c_send, c_recv, p_send, p_recv, out_sem,
):
    me = lax.axis_index("ctx")
    hme = lax.axis_index("head")
    dh = q_v.shape[1]
    cols = wo.shape[2]
    reach = WINDOW // rows
    scale = dh ** (-0.5) * LOG2E
    core = lax.rem(me, 2)
    fine = n <= 8
    evens = sorted(range(2, n, 2), key=lambda c: (bin(c).count("1"), c))
    hpair = hme // 2
    hodd = lax.rem(hme, 2)
    mate = hme + 1 - 2 * hodd

    def fetch(i, src, dst):
        copy = pltpu.make_async_copy(src, dst, load.at[i])
        copy.start()
        return copy

    first, second = pl.ds(0, rows), pl.ds(rows, rows)
    def fetch_rows(i, src, dst, parts):
        size = dst.shape[0] // parts
        for at in range(0, dst.shape[0], size):
            fetch(i, src.at[pl.ds(at, size)], dst.at[pl.ds(at, size)])
        return pltpu.make_async_copy(dst, dst, load.at[i])

    in_tok0 = fetch_rows(0, tok_h.at[first], tok.at[first], 2)
    in_k = fetch_rows(1, w_h.at[:, pl.ds(dh, dh)], w.at[1], 4)

    barrier = pltpu.get_barrier_semaphore()
    peers = [1] + evens
    for c in peers:
        pl.semaphore_signal(
            barrier, inc=1, device_id={"ctx": me ^ c}, device_id_type=pl.DeviceIdType.MESH
        )
    for r in range(1, nh):
        pl.semaphore_signal(
            barrier,
            inc=1,
            device_id={"head": lax.rem(hme + r, nh)},
            device_id_type=pl.DeviceIdType.MESH,
        )

    half = rows // 2
    slots = arrivals(n)

    def piece(b, c, sub, kv):
        span = pl.ds(b * rows, rows) if sub is None else pl.ds(b * rows + sub * half, half)
        return every.at[me ^ c, slice(None) if kv is None else kv, span]

    def slot(b, c, sub, kv):
        for key in ((b, c, sub, kv), (b, c, sub, None), (b, c, None, None)):
            if key in slots:
                return slots[key]

    def kv_copy(b, c, sub, kv, bit):
        ref = piece(b, c, sub, kv)
        return remote(
            ref, ref, k_send.at[b, sub], k_recv.at[slot(b, c | bit, sub, kv)], "ctx", me ^ bit
        )

    def kv_wait(b, c, sub=None, kv=None):
        ref = piece(b, c, sub, kv)
        at = k_recv.at[slot(b, c, sub, kv)]
        remote(ref, ref, k_send.at[0, 0], at, "ctx", me ^ (c & -c)).wait_recv()

    def pass_on(b, c, sub, kv):
        order = cross_bits(n, sub)
        last = max(i for i, bit in enumerate(order) if c & bit)
        for bit in order[last + 1 :] + [1]:
            kv_copy(b, c, sub, kv, bit).start()

    def send_own(b, kv, turns):
        for turn in turns:
            for sub in range(2):
                kv_copy(b, 0, sub, kv, cross_bits(n, sub)[turn]).start()
        if 0 in turns:
            for sub in range(2):
                kv_copy(b, 0, sub, kv, 1).start()

    def kv_sent():
        for b in range(2):
            for sub in range(2):
                ref = every.at[pl.ds(0, n - 1), :, pl.ds(0, half)]
                remote(
                    ref, ref, k_send.at[b, sub], k_recv.at[0], "ctx", me ^ 1
                ).wait_send()

    later_turns = range(1, len(cross_bits(n, 0)))

    def hops(b, far, first):
        for c in evens:
            for kv in range(2) if first else (None,):
                for sub in range(2):
                    near = c == cross_bits(n, sub)[0]
                    if far == (c & (c - 1) != 0) and (far or first == near):
                        kv_wait(b, c, sub, kv)
                        pass_on(b, c, sub, kv)

    def first_hops(b):
        hops(b, False, True)

    def near_hops(b):
        hops(b, False, False)

    def far_hops(b):
        hops(b, True, False)

    def from_mate(b, c):
        kv_wait(b, c)

    in_tok0.wait()
    in_k.wait()
    in_v = fetch_rows(2, w_h.at[:, pl.ds(2 * dh, dh)], w.at[2], 4)
    in_wr = fetch(7, wr_h, wr)
    in_gain = fetch(8, gain_h, gain)
    every[me, 0, :rows] = nn(tok[:rows], w[1]).astype(BF)
    pl.semaphore_wait(barrier, len(peers) + nh - 1)
    send_own(0, 0, (0,))
    in_v.wait()
    in_tok1 = fetch(3, tok_h.at[second], tok.at[second])
    in_q = fetch(4, w_h.at[:, pl.ds(0, dh)], w.at[0])
    for i, f in enumerate((f1_h, f3_h, f2_h)):
        fetch(5, f, f_v.at[i])
    in_f = pltpu.make_async_copy(f_v, f_v, load.at[5])
    for t in range(nh):
        fetch(6, wo_h.at[:, pl.ds(t * cols, cols)], wo.at[t])
    in_wo = pltpu.make_async_copy(wo, wo, load.at[6])
    every[me, 1, :rows] = nn(tok[:rows], w[2]).astype(BF)
    send_own(0, 1, (0,))
    send_own(0, None, later_turns)

    def rate_copy(c):
        i = c // 2
        return remote(rates.at[0], rates.at[i], s_send, s_recv, "ctx", me ^ c)

    in_wr.wait()
    logit = nt(jnp.broadcast_to(wr[...], (8, wr.shape[1])), tok[:rows])
    rates[0] = jnp.maximum(logit, 0.0) + jnp.log1p(jnp.exp(-jnp.abs(logit)))
    for c in evens:
        rate_copy(c).start()

    others = rates.at[pl.ds(1, n // 2 - 1)]
    all_rates = remote(others, others, s_send, s_recv, "ctx", me ^ 1)

    def crosses(h, t):
        odd = lax.rem(h, 2)
        up = (odd == 1) & (t // 2 > h // 2)
        down = (odd == 0) & (t // 2 < h // 2)
        return up | down

    share = pl.ds(pl.multiple_of(core * (dh // 2), dh // 2), dh // 2)

    def wo_copy(t):
        return remote(
            wo_h.at[share, pl.ds(t * cols, cols)],
            wp.at[t, share],
            w_send.at[0, t],
            w_recv.at[0, t],
            "head",
            mate,
        )

    def wo_pass(t):
        ref = wp.at[t, share]
        return remote(ref, ref, w_send.at[1, t], w_recv.at[1, t], "ctx", me ^ 1)

    def wo_gets(t):
        return (hme == t) | crosses(hme, t)

    for t in range(nh):

        @pl.when((mate == t) | crosses(mate, t))
        def _():
            wo_copy(t).start()

    in_tok1.wait()
    every[me, 0, rows:] = nn(tok[rows:], w[1]).astype(BF)
    every[me, 1, rows:] = nn(tok[rows:], w[2]).astype(BF)
    in_q.wait()
    in_gain.wait()
    q_v[...] = nn(tok[...], w[0]).astype(BF)
    in_f.wait()
    for i in range(3):
        fb[i] = f_v[i].astype(BF)

    def gradients(s, at, slot, add, close_sum=False):
        keys = every[s, 0, :rows]
        vals = every[s, 1, :rows]
        rate = jnp.transpose(rates[at])[:, :1]
        target = (-rate * vals.astype(F32)).astype(BF)
        h1 = nn(keys, fb[0])
        h3 = nn(keys, fb[1])
        sig = jax.nn.sigmoid(h1)
        silu = h1 * sig
        act = (silu * h3).astype(BF)
        dact = nt(target, fb[2])
        d1 = (dact * h3 * (sig * (1.0 + h1 * (1.0 - sig)))).astype(BF)
        d3 = (dact * silu).astype(BF)
        new = (tn(keys, d1), tn(keys, d3), tn(act, target))
        for i in range(3):
            if close_sum:
                grad[0, i] = grad[0, i] + (grad[1, i] + new[i])
            else:
                grad[slot, i] = grad[slot, i] + new[i] if add else new[i]

    def attend(b, sources, side, gap=None, begin=False, hide=None):
        q = q_v[pl.ds(pl.multiple_of(b * rows, rows), rows)]
        span = pl.ds(side * rows, rows)
        scores = [nt(q, every[s, 0, span]) for s in sources]
        if gap is not None:
            off = (
                lax.broadcasted_iota(jnp.int32, (rows, rows), 0)
                - lax.broadcasted_iota(jnp.int32, (rows, rows), 1)
                + gap * rows
            )
            scores = [jnp.where((off >= 0) & (off < WINDOW), sc, NEG) for sc in scores]
        if hide is not None:
            scores = [sc + bias for sc, bias in zip(scores, hide)]
        top = functools.reduce(jnp.maximum, scores)
        new = jnp.max(top, axis=1, keepdims=True)
        if not begin:
            new = jnp.maximum(m_s[b], new)
        probs = [jnp.exp2((sc - new) * scale) for sc in scores]
        lane = sum(p[:, i : i + LANES] for p in probs for i in range(0, rows, LANES))
        pv = sum(nn(p.astype(BF), every[s, 1, span]) for p, s in zip(probs, sources))
        if begin:
            l_s[b] = lane
            acc[b] = pv
        else:
            fade = jnp.exp2((m_s[b] - new) * scale)
            l_s[b] = l_s[b] * fade + lane
            acc[b] = acc[b] * fade + pv
        m_s[b] = new

    def visit(c):
        sources = [me ^ c] if c == 1 else [me ^ c, me ^ c ^ 1]
        attend(jnp.where(me > me ^ c, 0, 1), sources, 0)

    def visit_before(single, chips):
        sources = [me ^ c for c in single] + [me ^ c ^ i for c in chips for i in range(2)]
        attend(1, sources, 1, hide=[jnp.where(me > s, 0.0, NEG) for s in sources])

    def visit_all(side):
        def one(s, carry):
            gap = me - s
            b = jnp.where(gap >= 0, side, 1)
            gap = gap + (b - side) * n

            @pl.when((s != me) & (gap >= 0) & (gap <= reach))
            def _():
                attend(b, [s], side, gap)

            return carry

        lax.fori_loop(0, n, one, 0)

    def fast_out(b, weights):
        q = q_v[b * rows : (b + 1) * rows]
        h1 = nn(q, weights[0])
        h3 = nn(q, weights[1])
        act = (jax.nn.silu(h1) * h3).astype(BF)
        out = nn(act, weights[2])
        inv = lax.rsqrt(jnp.mean(out * out, axis=1, keepdims=True) + norm_eps)
        normed[...] = out * inv * gain[...]

    if fine:
        gradients(me, 0, 0, False)
    fast_out(0, fb)
    attend(0, [me], 0, 0, True)
    first_hops(0)
    for kv in range(2):
        send_own(1, kv, (0,))
    send_own(1, None, later_turns)
    attend(1, [me], 1, 0, True)
    if n <= reach:
        attend(1, [me], 0, n)
    from_mate(0, 1)
    if fine:
        visit(1)
    near_hops(0)
    all_rates.wait_recv()
    if fine:
        for c in evens:
            if c & (c - 1) == 0:
                gradients(me ^ c, c // 2, c // 4, c < 4)
        for c in evens:
            if c & (c - 1) == 0:
                from_mate(0, c + 1)
                visit(c)
    far_hops(0)
    if fine:
        for c in evens:
            if c & (c - 1):
                gradients(me ^ c, c // 2, 1, True, True)
    else:
        grad[0] = jnp.zeros_like(grad[0])

        def summed(j, carry):
            gradients(2 * j + core, (me // 2) ^ j, 0, True)
            return carry

        lax.fori_loop(0, n // 2, summed, 0)

    def g_copy(i):
        return remote(g_out.at[i], g_in.at[i], e_send.at[i], e_recv.at[i], "ctx", me ^ 1)

    def x_copy(i):
        return remote(g_out.at[i], g_in.at[i], e_send.at[i], e_recv.at[i], "ctx", me ^ 1)

    owned = ((0, 1), (2,))

    for own in range(2):

        @pl.when(core == own)
        def _():
            for i in owned[1 - own]:
                g_out[i] = grad[0, i].astype(BF)
                g_copy(i).start()

    chunks = comb.shape[2]
    pairs = nh // 2
    step = rows // chunks

    def c_copy(b, u):
        return remote(
            comb.at[b, 0, u], comb.at[b, 1, u], c_send.at[b], c_recv.at[b, u], "head", mate
        )

    def spot(b, u):
        return pl.ds(b * rows + u * step, step)

    def p_copy(b, u, t):
        return remote(
            tok.at[spot(b, u), pl.ds(t * cols, cols)],
            part_in.at[b, lax.rem(hpair - t // 2 + pairs, pairs) - 1, u],
            p_send.at[b, t],
            p_recv.at[b, u, lax.rem(hpair - t // 2 + pairs, pairs) - 1],
            "head",
            t,
        )

    def combine(b):
        both = acc[b] / jnp.sum(l_s[b], axis=1, keepdims=True) + normed[...]
        for u in range(chunks):
            comb[b, 0, u] = both[u * step : (u + 1) * step].astype(BF)
            c_copy(b, u).start()

    targets = sorted(range(nh), key=lambda t: -abs(2 * t - nh + 1))

    def cross(b):
        if b == 0:
            for u in range(chunks):
                c_copy(b, u).wait_recv()
        for t in targets:

            @pl.when(crosses(hme, t))
            def _():
                if b == 0:
                    mine, pair = (comb[b, k].reshape(rows, dh) for k in range(2))
                    tok[b * rows : (b + 1) * rows, t * cols : (t + 1) * cols] = (
                        nn(mine, wo[t]) + nn(pair, wp[t])
                    ).astype(BF)
                for u in range(chunks):
                    if b > 0:
                        if t == 0 or t == nh - 1:
                            c_copy(b, u).wait_recv()
                        tok[spot(b, u), t * cols : (t + 1) * cols] = (
                            nn(comb[b, 0, u], wo[t]) + nn(comb[b, 1, u], wp[t])
                        ).astype(BF)
                    p_copy(b, u, t).start()

    def own_part(b):
        if b > 0:

            @pl.when(jnp.logical_not(crosses(hme, 0) | crosses(hme, nh - 1)))
            def _():
                for u in range(chunks):
                    c_copy(b, u).wait_recv()

        mine, pair = (comb[b, k].reshape(rows, dh) for k in range(2))
        res[b] = nn(mine, wo[hme]) + nn(pair, wp[hme])

    def close(b):
        for u in range(chunks):
            for pair in range(pairs - 1):
                ref = part_in.at[b, pair, u]
                remote(ref, ref, p_send.at[b, 0], p_recv.at[b, u, pair], "head", mate).wait_recv()
                here = slice(u * step, (u + 1) * step)
                res[b, here] = res[b, here] + part_in[b, pair, u].astype(F32)

        q_v[b * rows : (b + 1) * rows] = res[b].astype(BF)
        copy = pltpu.make_async_copy(
            q_v.at[pl.ds(b * rows, rows)], mixed_h.at[b], out_sem.at[1 + b]
        )
        copy.start()
        return copy

    for t in range(nh):

        @pl.when(wo_gets(t))
        def _():
            wo_copy(t).wait_recv()
            wo_pass(t).start()

    if fine:
        for c in evens:
            if c & (c - 1):
                from_mate(0, c + 1)
                visit(c)
    else:
        for c in evens:
            from_mate(0, c + 1)
        visit_all(0)
    combine(0)

    def ns_step(i, norm=None):
        x = grad[0, i]
        xb = x.astype(BF)
        gram = nt(xb, xb)
        if norm is not None:
            gram = gram * (norm * norm)
        gb = gram.astype(BF)
        poly = coeff_b * gram + coeff_c * nn(gb, gb)
        new = coeff_a * x + nn(poly.astype(BF), xb)
        grad[0, i] = new if norm is None else new * norm

    def ns_steps(mats, count):
        def one(_, carry):
            for i in mats:
                ns_step(i)
            return carry

        lax.fori_loop(0, count, one, 0)

    for own in range(2):

        @pl.when(core == own)
        def _():
            for i in owned[own]:
                g_copy(i).wait_recv()
            norms = []
            for i in owned[own]:
                g = grad[0, i] + g_in[i].astype(F32)
                grad[0, i] = g
                norms.append(lax.rsqrt(jnp.sum(g * g) + norm_eps))
            for i, norm in zip(owned[own], norms):
                ns_step(i, norm)

    for count in range(2):
        if count == 1:
            first_hops(1)
        for own in range(2):

            @pl.when(core == own)
            def _():
                ns_steps(owned[own], 1)

    for own in range(2):

        @pl.when(core == own)
        def _():
            ns_steps(owned[own], NS_STEPS - 4)

    near_hops(1)
    for t in range(nh):

        @pl.when(wo_gets(t))
        def _():
            wo_pass(t).wait_recv()

    in_wo.wait()
    cross(0)
    for own in range(2):

        @pl.when(core == own)
        def _():
            for i in owned[own]:
                ns_step(i)
                g_out[i] = grad[0, i].astype(BF)
                x_copy(i).start()

    def second(far):
        chips = [c for c in evens if far == (c & (c - 1) != 0)]
        for c in chips:
            from_mate(1, c + 1)
        visit_before([] if far else [1], chips)

    from_mate(1, 1)

    if fine:
        second(False)
    far_hops(1)

    def stepped(own, i):
        moved = g_out[i] if i in owned[own] else g_in[i]
        return f_v[i] - fast_step * moved.astype(F32)

    for own in range(2):

        @pl.when(core == own)
        def _():
            for i in owned[1 - own]:
                x_copy(i).wait_recv()
            for i in range(3):
                fb[i] = stepped(own, i).astype(BF)

    if fine:
        fast_out(1, fb)
        second(True)
        combine(1)
    else:
        fast_out(1, fb)
        for c in evens:
            from_mate(1, c + 1)
        visit_all(1)
        combine(1)
    for own in range(2):

        @pl.when(core == own)
        def _():
            for i in range(3):
                f_v[i] = stepped(own, i)

    outs = (o1_h, o3_h, o2_h)
    writes = [pltpu.make_async_copy(f_v.at[i], outs[i], out_sem.at[0]) for i in range(3)]
    for copy in writes:
        copy.start()
    writes = [pltpu.make_async_copy(f_v, f_v, out_sem.at[0])]
    own_part(0)
    cross(1)
    own_part(1)
    writes.append(close(0))
    writes.append(close(1))
    for copy in writes:
        copy.wait()
    kv_sent()
    all_rates.wait_send()
    for b in range(2):
        ref = comb.at[b, 0]
        remote(ref, ref, c_send.at[b], c_recv.at[b, 0], "head", mate).wait_send()
    for own in range(2):

        @pl.when(core == own)
        def _():
            for i in owned[1 - own]:
                g_copy(i).wait_send()
            for i in owned[own]:
                x_copy(i).wait_send()

    for t in range(nh):

        @pl.when((mate == t) | crosses(mate, t))
        def _():
            wo_copy(t).wait_send()

        @pl.when(wo_gets(t))
        def _():
            wo_pass(t).wait_send()

        @pl.when(crosses(hme, t))
        def _():
            for b in range(2):
                ref = tok.at[pl.ds(b * rows, rows), pl.ds(t * cols, cols)]
                remote(ref, ref, p_send.at[b, t], p_recv.at[0, 0, 0], "head", mate).wait_send()


def layer(n, nh, rows, flat, w_qkv, w_rate, f1, f3, f2, gain, wo):
    total, width = flat.shape
    blocks = total // rows
    dh, fh = f1.shape
    cols = wo.shape[1] // nh
    chunks = 4
    step = rows // chunks
    dma = pltpu.SemaphoreType.DMA
    buffers = [
        pltpu.VMEM((total, width), BF),
        pltpu.VMEM((3, width, dh), BF),
        pltpu.VMEM((1, width), BF),
        pltpu.VMEM((1, dh), F32),
        pltpu.VMEM((3, dh, fh), F32),
        pltpu.VMEM((3, dh, fh), BF),
        pltpu.VMEM((nh, dh, cols), BF),
        pltpu.VMEM((nh, dh, cols), BF),
        pltpu.VMEM((total, dh), BF),
        pltpu.VMEM((n, 2, total, dh), BF),
        pltpu.VMEM((n // 2, 8, rows), F32),
        pltpu.VMEM((2 if n <= 8 else 1, 3, dh, fh), F32),
        pltpu.VMEM((3, dh, fh), BF),
        pltpu.VMEM((3, dh, fh), BF),
        pltpu.VMEM((blocks, rows, 1), F32),
        pltpu.VMEM((blocks, rows, LANES), F32),
        pltpu.VMEM((blocks, rows, dh), F32),
        pltpu.VMEM((rows, dh), F32),
        pltpu.VMEM((blocks, 2, chunks, step, dh), BF),
        pltpu.VMEM((blocks, nh // 2 - 1, chunks, step, cols), BF),
        pltpu.VMEM((blocks, rows, cols), F32),
    ]
    need = sum(math.prod(b.shape) * jnp.dtype(b.dtype).itemsize for b in buffers)
    return pl.pallas_call(
        functools.partial(layer_kernel, n, nh, rows),
        in_specs=[HBM] * 8,
        out_specs=[ANY] * 4,
        out_shape=[jax.ShapeDtypeStruct((blocks, rows, cols), BF)]
        + [jax.ShapeDtypeStruct(f.shape, F32) for f in (f1, f3, f2)],
        scratch_shapes=[
            *buffers,
            dma((9,)),
            dma((blocks, 2)),
            dma((len(arrivals(n)),)),
            dma,
            dma,
            dma((3,)),
            dma((3,)),
            dma((2, nh)),
            dma((2, nh)),
            dma((blocks,)),
            dma((blocks, chunks)),
            dma((blocks, nh)),
            dma((blocks, chunks, nh // 2 - 1)),
            dma((1 + blocks,)),
        ],
        compiler_params=pltpu.CompilerParams(
            vmem_limit_bytes=min(67_000_000, need + 6_000_000), collective_id=0, has_side_effects=True
        ),
        name="layer",
    )(
        *(
            pltpu.with_memory_space_constraint(x, pltpu.HBM)
            for x in (flat, w_qkv, w_rate, f1, f3, f2, gain, wo)
        )
    )


def write_kernel(*refs):
    half = len(refs) // 2
    sems = refs[-1]
    for i in range(half):
        size = refs[i].shape[-2] // 2
        for at in range(2):
            span = (slice(None),) * (len(refs[i].shape) - 2) + (pl.ds(at * size, size),)
            pltpu.make_async_copy(refs[i].at[span], refs[half + i].at[span], sems.at[i]).start()
    for i in range(half):
        pltpu.make_async_copy(refs[i], refs[half + i], sems.at[i]).wait()


def write_out(arrays):
    return pl.pallas_call(
        write_kernel,
        in_specs=[ANY] * len(arrays),
        out_specs=[HBM] * len(arrays),
        out_shape=[jax.ShapeDtypeStruct(a.shape, a.dtype) for a in arrays],
        scratch_shapes=[pltpu.SemaphoreType.DMA((len(arrays),))],
        compiler_params=pltpu.CompilerParams(vmem_limit_bytes=4_000_000),
        name="write_out",
    )(*arrays)


def shards(tokens, w_qkv, w_rate, w_out, fw_gain, fast_first, fast_third, fast_second):
    blocks, rows, width = tokens.shape
    dh = w_out.shape[1]
    done = layer(
        lax.axis_size("ctx"),
        lax.axis_size("head"),
        rows,
        tokens.reshape(blocks * rows, width),
        w_qkv.reshape(width, 3 * dh),
        w_rate.reshape(1, width),
        fast_first[0],
        fast_third[0],
        fast_second[0],
        fw_gain,
        w_out[0],
    )
    mixed, *current = write_out(done)
    return (mixed,) + tuple(f[None] for f in current)


def solution(mesh):
    placed = (
        P(None, "ctx", None),
        P(None, "head", None),
        P(None, "head"),
        P("head", None, None),
        P("head", None),
        P("head", None, None),
        P("head", None, None),
        P("head", None, None),
    )
    return jax.shard_map(
        shards,
        mesh=mesh,
        in_specs=placed,
        out_specs=(
            P(None, "ctx", "head"),
            P("head", None, None),
            P("head", None, None),
            P("head", None, None),
        ),
        check_vma=False,
    )
```
